32 devices in a mesh: seq: 16 (over z, y, x), head: 2 (over core).
Axes of the slice: x: 2, y: 2, z: 4, core: 2. Of those that a mesh axis runs over, the one named last changes fastest.
Arguments:
- hidden_state_input: bfloat16 [16, 8192], P(None, 'seq'), may hold values from -40 to 40
- attention_norm_gain: bfloat16 [8192], P('seq'), may hold values from 0.099609375 to 1.8984375
- query_projection_matrix: bfloat16 [8192, 8192], P('seq', 'head'), may hold values from -0.0625 to 0.0625
- key_projection_matrix: bfloat16 [8192, 1024], P('seq', 'head'), may hold values from -0.0625 to 0.0625
- value_projection_matrix: bfloat16 [8192, 1024], P('seq', 'head'), may hold values from -0.0625 to 0.0625
- output_projection_matrix: bfloat16 [8192, 8192], P('head', 'seq'), may hold values from -0.25 to 0.25
- adapter_down_matrix: bfloat16 [512, 16, 8192], P('head', None, 'seq'), may hold values from -0.0625 to 0.0625
- adapter_up_matrix: bfloat16 [512, 16, 8192], P('seq', None, 'head'), may hold values from -3 to 3
- adapter_choice_index: int32 [16], replicated, may hold values from 0 to 511
- lengths: int32 [16], replicated, may hold values from 4 to 4096
- rotated_key_cache: bfloat16 [16, 4096, 8, 128], P(None, 'seq', 'head'), may hold values from -200 to 200
- cached_value_rows: bfloat16 [16, 4096, 8, 128], P(None, 'seq', 'head'), may hold values from -24 to 24
Outputs:
- output_sum: bfloat16 [16, 8192], P(None, 'seq')
The draws below stay inside these ranges and needn't reach their ends.
Inputs may be any that keep to these rules, and one draw needn't show every extreme that they name: `adapter_choice_index`: index of the adapter that serves each request. The new token stands at position lengths[r]; cache entries at lengths[r] and beyond are not read.
All inputs are finite; a program needn't handle non-finite values.
Results may differ from the reference program's by a relative error of at most 0.025.
Values may be sent and summed in bfloat16 or wider, within the bound.
No kernel may reach another device: no remote copies, remote signals or barrier semaphores. Data moves between devices by JAX's collectives and lax.ppermute only.
A program may use at most 64 MiB of HBM per device.

```python
import math
import jax
import jax.numpy as jnp
from jax import lax

MODEL_DIMENSION = 8192
QUERY_HEADS = 64
KVH = 8
HEAD_SIZE = 128
ADAPTER_COUNT = 512
ADAPTER_RANK = 16
REQ = 16
CONTEXT = 4096


def draw_hidden_state_input(key, part):
    key_noise, key_rows, key_cols = jax.random.split(key, 3)
    jitter = jax.random.normal(key_noise, (REQ, MODEL_DIMENSION), jnp.float32)
    lowest = math.log(0.3)
    row_scale = jnp.exp(jax.random.uniform(key_rows, (REQ, 1), jnp.float32, lowest, math.log(3.0)))
    col_scale = jnp.exp(jax.random.uniform(key_cols, (1, MODEL_DIMENSION), jnp.float32, 0.0, math.log(10.0)))
    rising = jnp.exp(jnp.arange(MODEL_DIMENSION, dtype=jnp.float32) * (math.log(3.0) / MODEL_DIMENSION))[None, :]
    return jnp.clip(0.25 * jitter * row_scale * col_scale * rising, -40.0, 40.0).astype(jnp.bfloat16)


def draw_rotated_key_cache(key, part):
    key_base = jax.random.fold_in(key, 0)
    shape_all = (REQ, CONTEXT, KVH, HEAD_SIZE)
    sample = jax.random.normal(key_base, shape_all, jnp.float32)
    return jnp.clip(sample, -200.0, 200.0).astype(jnp.bfloat16)


def plant(drawn, key, low, top_value):
    longest = drawn.shape.index(max(drawn.shape))
    spots = []
    for shift in (0, 1):
        where = [jax.random.randint(jax.random.fold_in(key, axis), (), 0, length) for axis, length in enumerate(drawn.shape)]
        where[longest] = (where[longest] + shift) % drawn.shape[longest]
        spots.append(tuple(where))
    return drawn.at[spots[0]].set(low).at[spots[1]].set(top_value)


def block_scale(rng, dims, shards, smallest, top_value):
    def one(dim, shards_of):
        draws = jax.random.uniform(jax.random.fold_in(jax.random.fold_in(rng, 6), dim), (shards_of,), jnp.float32, smallest / len(shards), top_value / len(shards))
        return jnp.repeat(jnp.exp(draws), dims[dim] // shards_of).reshape((-1,) + (1,) * (len(dims) - dim - 1))

    factor_of = one(*shards[0])
    for cut in shards[1:]:
        factor_of = factor_of * one(*cut)
    return factor_of


def bell_draw(key, shape, width, reach, pieces=(), kind=jnp.bfloat16):
    entries = width * jax.random.normal(key, shape, jnp.float32)
    if pieces:
        entries = entries * block_scale(key, shape, pieces, -0.22, 0.18)
    return jnp.clip(entries, -reach, reach).astype(kind)


def setup_inputs(seed: int = 0) -> dict:
    key_of = jax.random.split(jax.random.key(seed), 13)
    return {
        "hidden_state_input": draw_hidden_state_input(jax.random.fold_in(key_of[12], 71), 0),
        "attention_norm_gain": jnp.clip(1.0 + 0.18 * jax.random.normal(key_of[1], (MODEL_DIMENSION,), jnp.float32), 0.099609375, 1.8984375).astype(jnp.bfloat16),
        "query_projection_matrix": bell_draw(key_of[2], (MODEL_DIMENSION, QUERY_HEADS * HEAD_SIZE), MODEL_DIMENSION ** -0.5, 0.0625, ((0, 16), (1, 2))),
        "key_projection_matrix": bell_draw(key_of[3], (MODEL_DIMENSION, KVH * HEAD_SIZE), MODEL_DIMENSION ** -0.5, 0.0625, ((0, 16), (1, 2))),
        "value_projection_matrix": bell_draw(key_of[4], (MODEL_DIMENSION, KVH * HEAD_SIZE), MODEL_DIMENSION ** -0.5, 0.0625, ((0, 16), (1, 2))),
        "output_projection_matrix": bell_draw(key_of[5], (QUERY_HEADS * HEAD_SIZE, MODEL_DIMENSION), (QUERY_HEADS * HEAD_SIZE // 16) ** -0.5, 0.25, ((0, 2), (1, 16))),
        "adapter_down_matrix": bell_draw(key_of[6], (ADAPTER_COUNT, ADAPTER_RANK, MODEL_DIMENSION), MODEL_DIMENSION ** -0.5, 0.0625, ((0, 2), (2, 16))),
        "adapter_up_matrix": bell_draw(key_of[7], (ADAPTER_COUNT, ADAPTER_RANK, QUERY_HEADS * HEAD_SIZE), (ADAPTER_RANK // 4) ** -0.5, 3.0, ((0, 16), (2, 2))),
        "adapter_choice_index": plant(jax.random.randint(key_of[8], (REQ,), 0, ADAPTER_COUNT), jax.random.fold_in(key_of[8], 1), 0, ADAPTER_COUNT - 1).astype(jnp.int32),
        "lengths": plant(jax.random.randint(key_of[9], (REQ,), 4, CONTEXT + 1), jax.random.fold_in(key_of[9], 1), 4, CONTEXT).astype(jnp.int32),
        "rotated_key_cache": draw_rotated_key_cache(jax.random.fold_in(key_of[12], 71), 0),
        "cached_value_rows": bell_draw(key_of[11], (REQ, CONTEXT, KVH, HEAD_SIZE), 4.0, 24.0, ((1, 16), (2, 2))),
    }


norm_epsilon = 1e-05
adapter_scale_factor = 1.0
rope_base = 500000.0
masked_score = -1e+30

def rotate(vectors, positions):
    half_dim = vectors.shape[-1] // 2
    frequency = jnp.exp(-jnp.arange(half_dim, dtype=jnp.float32) * (jnp.log(jnp.float32(rope_base)) / half_dim))
    angles = positions.astype(jnp.float32)[:, None] * frequency[None, :]
    cosine = jnp.cos(angles)[:, None, :]
    sine_val = jnp.sin(angles)[:, None, :]
    lower_half = vectors[..., :half_dim]
    upper_half = vectors[..., half_dim:]
    return jnp.concatenate([lower_half * cosine - upper_half * sine_val, upper_half * cosine + lower_half * sine_val], axis=-1)

def reference(hidden_state_input, attention_norm_gain, query_projection_matrix, key_projection_matrix, value_projection_matrix, output_projection_matrix, adapter_down_matrix, adapter_up_matrix, adapter_choice_index, lengths, rotated_key_cache, cached_value_rows):
    values32 = hidden_state_input.astype(jnp.float32)
    inverse_factor = lax.rsqrt(lax.optimization_barrier(jnp.mean(values32 * values32, axis=1)) + norm_epsilon)
    scaled = (values32 * attention_norm_gain.astype(jnp.float32)[None, :]).astype(jnp.bfloat16)
    scaled_wide_query = lax.optimization_barrier(scaled).astype(jnp.float32)
    down_map_rows = adapter_down_matrix[adapter_choice_index].astype(jnp.float32)
    reduced_rank_state = (jnp.einsum('by,bey->be', scaled_wide_query, down_map_rows) * inverse_factor[:, None] * adapter_scale_factor).astype(jnp.bfloat16)
    shrunk_wide = lax.optimization_barrier(reduced_rank_state).astype(jnp.float32)
    up_map_rows = adapter_up_matrix[adapter_choice_index].astype(jnp.float32)
    query_full = jnp.dot(scaled, query_projection_matrix, preferred_element_type=jnp.float32) * inverse_factor[:, None] + jnp.einsum('rk,rkc->rc', shrunk_wide, up_map_rows)
    key_new = jnp.dot(scaled, key_projection_matrix, preferred_element_type=jnp.float32) * inverse_factor[:, None]
    value_new = jnp.dot(scaled, value_projection_matrix, preferred_element_type=jnp.float32) * inverse_factor[:, None]
    query_rot = rotate(query_full.reshape(REQ, QUERY_HEADS, HEAD_SIZE), lengths).astype(jnp.bfloat16)
    key_rot = rotate(key_new.reshape(REQ, KVH, HEAD_SIZE), lengths).astype(jnp.bfloat16)
    value_own = value_new.reshape(REQ, KVH, HEAD_SIZE).astype(jnp.bfloat16)
    grouped = query_rot.reshape(REQ, KVH, QUERY_HEADS // KVH, HEAD_SIZE)
    score_scale = HEAD_SIZE ** (-0.5)

    def one_request(request_items):
        query_one, key_rows, value_rows, length, own_key, own_value = request_items
        query_wide = query_one.astype(jnp.float32)
        scores = jnp.einsum('hgd,jhd->hgj', query_wide, key_rows.astype(jnp.float32)) * score_scale
        valid_mask = jnp.arange(CONTEXT) < length
        scores = jnp.where(valid_mask[None, None, :], scores, masked_score)
        own_score = jnp.einsum('hgd,hd->hg', query_wide, own_key.astype(jnp.float32)) * score_scale
        peak = jnp.maximum(lax.optimization_barrier(jnp.max(scores, axis=-1)), own_score)
        weights = jnp.where(valid_mask[None, None, :], jnp.exp(scores - peak[..., None]), 0.0)
        own_weight = jnp.exp(own_score - peak)
        denominator = lax.optimization_barrier(jnp.sum(weights, axis=-1)) + own_weight
        probs = lax.optimization_barrier(weights.astype(jnp.bfloat16)).astype(jnp.float32)
        summed = jnp.einsum('hgj,jhd->hgd', probs, value_rows.astype(jnp.float32))
        summed = summed + own_weight[..., None] * own_value.astype(jnp.float32)[:, None, :]
        return (summed / denominator[..., None]).astype(jnp.bfloat16)
    attended = lax.map(one_request, (grouped, rotated_key_cache, cached_value_rows, lengths, key_rot, value_own))
    attended = attended.reshape(REQ, QUERY_HEADS * HEAD_SIZE)
    return jnp.dot(attended, output_projection_matrix, preferred_element_type=jnp.float32).astype(jnp.bfloat16)
```

```python
import jax
import jax.numpy as jnp
from jax import lax
from jax.sharding import PartitionSpec as P

norm_epsilon = 1e-05
adapter_scale_factor = 1.0
rope_base = 500000.0
masked_score = -1e30


def exchanged(parts):
    return lax.all_to_all(parts, "seq", 0, 0, tiled=True)


def spread(value):
    return exchanged(jnp.broadcast_to(value[None], (lax.axis_size("seq"),) + value.shape))


def narrow(value):
    return lax.reduce_precision(value, exponent_bits=8, mantissa_bits=7)


def rotate(vectors, cosine, sine_val):
    half_dim = vectors.shape[-1] // 2
    lower_half = vectors[..., :half_dim]
    upper_half = vectors[..., half_dim:]
    return jnp.concatenate(
        [lower_half * cosine - upper_half * sine_val, upper_half * cosine + lower_half * sine_val],
        axis=-1,
    )


def angle_tables(positions, half_dim):
    frequency = jnp.exp(
        -jnp.arange(half_dim, dtype=jnp.float32) * (jnp.log(jnp.float32(rope_base)) / half_dim)
    )
    angles = positions.astype(jnp.float32)[:, None] * frequency[None, :]
    return jnp.cos(angles), jnp.sin(angles)


def body(
    hidden_state_input,
    attention_norm_gain,
    query_projection_matrix,
    key_projection_matrix,
    value_projection_matrix,
    output_projection_matrix,
    adapter_down_matrix,
    adapter_up_matrix,
    adapter_choice_index,
    lengths,
    rotated_key_cache,
    cached_value_rows,
):
    requests = hidden_state_input.shape[0]
    width_part = hidden_state_input.shape[1]
    cached = rotated_key_cache.shape[1]
    kv_local = rotated_key_cache.shape[2]
    head_dim = rotated_key_cache.shape[3]
    query_cols = query_projection_matrix.shape[1]
    heads_local = query_cols // head_dim
    group_size = heads_local // kv_local
    rank = adapter_down_matrix.shape[1]
    seq_index = lax.axis_index("seq")
    head_index = lax.axis_index("head")
    seq_size = lax.axis_size("seq")
    head_size = lax.axis_size("head")
    model_width = width_part * seq_size
    score_scale = head_dim ** (-0.5)
    own_rows = requests * heads_local // seq_size
    if own_rows % group_size == 0:
        own_kv, kv_repeat = own_rows // group_size, 1
    else:
        own_kv, kv_repeat = 1, group_size // own_rows

    values32 = hidden_state_input.astype(jnp.float32)
    square_part = jnp.sum(values32 * values32, axis=1)
    square_part = jnp.where(head_index == 0, square_part, 0.0)
    scaled = (values32 * attention_norm_gain.astype(jnp.float32)[None, :]).astype(jnp.bfloat16)
    down_row_count = adapter_down_matrix.shape[0]
    resident_down_map = adapter_choice_index - head_index * down_row_count
    down_owned = (resident_down_map >= 0) & (resident_down_map < down_row_count)
    down_map_rows = adapter_down_matrix[jnp.clip(resident_down_map, 0, down_row_count - 1)]
    down_part = jnp.einsum("by,bey->be", scaled, down_map_rows, preferred_element_type=jnp.float32)
    down_part = jnp.where(down_owned[:, None], down_part, 0.0)

    small = jnp.concatenate([down_part.reshape(-1), square_part])
    small = jnp.pad(small, (0, -small.shape[0] % 128))
    everyone = seq_size * head_size
    small = lax.all_to_all(
        jnp.broadcast_to(small[None], (everyone,) + small.shape), ("seq", "head"), 0, 0, tiled=True
    )
    small = jnp.sum(small, axis=0)
    down_total_sum = small[: requests * rank].reshape(requests, rank)
    square_sum = small[requests * rank : requests * rank + requests]
    inverse_factor = lax.rsqrt(square_sum / model_width + norm_epsilon)
    reduced_rank_state = (down_total_sum * inverse_factor[:, None] * adapter_scale_factor).astype(
        jnp.bfloat16
    )

    up_row_count = adapter_up_matrix.shape[0]
    resident_up_map = adapter_choice_index - seq_index * up_row_count
    up_owned = (resident_up_map >= 0) & (resident_up_map < up_row_count)
    up_map_rows = adapter_up_matrix[jnp.clip(resident_up_map, 0, up_row_count - 1)]
    expand = jnp.einsum(
        "rk,rkc->rc", reduced_rank_state, up_map_rows, preferred_element_type=jnp.float32
    )
    expand = jnp.where(up_owned[:, None], expand, 0.0)
    query_part = jnp.dot(scaled, query_projection_matrix, preferred_element_type=jnp.float32)
    key_part = jnp.dot(scaled, key_projection_matrix, preferred_element_type=jnp.float32)
    value_part = jnp.dot(scaled, value_projection_matrix, preferred_element_type=jnp.float32)
    query_part = query_part * inverse_factor[:, None] + expand
    key_part = key_part * inverse_factor[:, None]
    value_part = value_part * inverse_factor[:, None]

    def kv_parts(part):
        rows = part.astype(jnp.bfloat16).reshape(-1, head_dim)
        return jnp.repeat(rows, kv_repeat, axis=0).reshape(seq_size, own_kv, head_dim)

    sums = exchanged(
        jnp.concatenate(
            [
                query_part.astype(jnp.bfloat16).reshape(seq_size, own_rows, head_dim),
                kv_parts(key_part),
                kv_parts(value_part),
            ],
            axis=1,
        )
    )
    sums = jnp.sum(sums.astype(jnp.float32), axis=0)
    query_row_request = (seq_index * own_rows + jnp.arange(own_rows)) // heads_local
    kv_row_request = query_row_request.reshape(own_kv, -1)[:, 0]
    cosine, sine_val = angle_tables(lengths[query_row_request], head_dim // 2)
    query_rot = rotate(sums[:own_rows], cosine, sine_val).astype(jnp.bfloat16)
    cosine, sine_val = angle_tables(lengths[kv_row_request], head_dim // 2)
    key_rot = rotate(sums[own_rows : own_rows + own_kv], cosine, sine_val).astype(jnp.bfloat16)
    value_own = sums[own_rows + own_kv :].astype(jnp.bfloat16)

    grouped = spread(query_rot).reshape(requests, kv_local, group_size, head_dim)
    scores = (
        jnp.einsum(
            "rhgd,rjhd->rhgj", grouped, rotated_key_cache, preferred_element_type=jnp.float32
        )
        * score_scale
    )
    position = seq_index * cached + jnp.arange(cached, dtype=jnp.int32)
    valid_mask = (position[None, :] < lengths[:, None])[:, None, None, :]
    scores = jnp.where(valid_mask, scores, masked_score)
    local_max = jnp.max(scores, axis=-1)
    shift_high = narrow(local_max)
    shift_low = narrow(local_max - shift_high)
    shift = shift_high + shift_low
    weights = jnp.where(valid_mask, jnp.exp(scores - shift[..., None]), 0.0)
    local_total = jnp.sum(weights, axis=-1)
    total_high = narrow(local_total)
    total_low = narrow(local_total - total_high)
    local_out = jnp.einsum(
        "rhgj,rjhd->rhgd",
        weights.astype(jnp.bfloat16),
        cached_value_rows,
        preferred_element_type=jnp.float32,
    )
    stats = jnp.stack(
        [
            piece.reshape(seq_size, own_rows)
            for piece in (shift_high, shift_low, total_high, total_low)
        ],
        axis=1,
    ).reshape(seq_size, 4 * own_rows)
    stats = jnp.pad(stats, ((0, 0), (0, -stats.shape[1] % head_dim)))
    stat_rows = stats.shape[1] // head_dim
    parts = exchanged(
        jnp.concatenate(
            [
                local_out.astype(jnp.bfloat16).reshape(seq_size, own_rows, head_dim),
                stats.astype(jnp.bfloat16).reshape(seq_size, stat_rows, head_dim),
            ],
            axis=1,
        )
    ).astype(jnp.float32)
    outs = parts[:, :own_rows]
    stats = parts[:, own_rows:].reshape(seq_size, -1)[:, : 4 * own_rows]
    stats = stats.reshape(seq_size, 4, own_rows)
    shifts = stats[:, 0] + stats[:, 1]
    totals = stats[:, 2] + stats[:, 3]

    own_group = own_rows // own_kv
    query_own = query_rot.astype(jnp.float32).reshape(own_kv, own_group, head_dim)
    own_score = jnp.sum(query_own * key_rot.astype(jnp.float32)[:, None, :], axis=-1) * score_scale
    own_score = own_score.reshape(own_rows)
    overall = jnp.maximum(jnp.max(shifts, axis=0), own_score)
    factor = jnp.exp(shifts - overall[None, :])
    own_weight = jnp.exp(own_score - overall)
    denominator = jnp.sum(totals * factor, axis=0) + own_weight
    own_value = jnp.broadcast_to(
        value_own.astype(jnp.float32)[:, None, :], (own_kv, own_group, head_dim)
    ).reshape(own_rows, head_dim)
    summed = jnp.sum(outs * factor[..., None], axis=0) + own_weight[:, None] * own_value
    attended = (summed / denominator[:, None]).astype(jnp.bfloat16)

    attended = spread(attended).reshape(requests, query_cols)
    out_part = jnp.dot(attended, output_projection_matrix, preferred_element_type=jnp.float32)
    if head_size == 2:
        output_sum = out_part + lax.ppermute(out_part, "head", [(0, 1), (1, 0)])
    else:
        output_sum = lax.psum(out_part, "head")
    return output_sum.astype(jnp.bfloat16)


def solution(mesh):
    return jax.shard_map(
        body,
        mesh=mesh,
        in_specs=(
            P(None, "seq"),
            P("seq"),
            P("seq", "head"),
            P("seq", "head"),
            P("seq", "head"),
            P("head", "seq"),
            P("head", None, "seq"),
            P("seq", None, "head"),
            P(),
            P(),
            P(None, "seq", "head", None),
            P(None, "seq", "head", None),
        ),
        out_specs=P(None, "seq"),
        check_vma=False,
    )
```

```python
import functools
import math

import jax
import jax.numpy as jnp
from jax import lax
from jax.experimental import pallas as pl
from jax.experimental.pallas import tpu as pltpu
from jax.sharding import PartitionSpec as P

norm_epsilon = 1e-05
adapter_scale_factor = 1.0
rope_base = 500000.0
masked_score = -1e30

IN_VMEM = pl.BlockSpec(memory_space=pltpu.VMEM)
IN_PLACE = pl.BlockSpec(memory_space=pltpu.HBM)


def exchanged(parts):
    return lax.all_to_all(parts, "seq", 0, 0, tiled=True)


def iota(shape, axis):
    return lax.broadcasted_iota(jnp.int32, shape, axis)


def rounded(value):
    return value.astype(jnp.bfloat16).astype(jnp.float32)


def started(source, target, sem):
    copy = pltpu.make_async_copy(source, target, sem)
    copy.start()
    return copy


def owned_column(choice_ref, first, count):
    requests = choice_ref.shape[0]
    row = iota((requests, 1), 0)
    column = jnp.zeros((requests, 1), jnp.int32)
    for r in range(requests):
        local = choice_ref[r] - first
        held = ((local >= 0) & (local < count)).astype(jnp.int32)
        column = jnp.where(row == r, held, column)
    return column > 0


def small_sums_kernel(
    choice_hbm,
    hidden_hbm,
    gain_hbm,
    down_ref,
    message_ref,
    scaled_ref,
    choice_ref,
    hidden_ref,
    gain_ref,
    rows_ref,
    sems,
):
    requests, rank, width = rows_ref.shape
    count = down_ref.shape[0]
    head_index = lax.axis_index("head")
    first = head_index * count
    choice_copy = started(choice_hbm, choice_ref, sems.at[requests])
    hidden_copy = started(hidden_hbm, hidden_ref, sems.at[requests + 1])
    gain_copy = started(gain_hbm, gain_ref, sems.at[requests + 2])
    choice_copy.wait()
    copies = []
    for r in range(requests):
        local = jnp.clip(choice_ref[r] - first, 0, count - 1)
        copies.append(started(down_ref.at[local], rows_ref.at[r], sems.at[r]))
    hidden_copy.wait()
    gain_copy.wait()
    values = hidden_ref[...].astype(jnp.float32)
    gain = gain_ref[...].astype(jnp.float32).reshape(1, width)
    scaled = (values * gain).astype(jnp.bfloat16)
    scaled_ref[...] = scaled
    squares = jnp.sum(values * values, axis=1, keepdims=True)
    squares = jnp.where(head_index == 0, squares, 0.0)
    diagonal = iota((requests, 128), 1) == iota((requests, 128), 0)
    squares = jnp.sum(jnp.where(diagonal, squares, 0.0), axis=0, keepdims=True)
    owned = owned_column(choice_ref, first, count)
    for copy in copies:
        copy.wait()
    products = lax.dot_general(
        scaled,
        rows_ref[...].reshape(requests * rank, width),
        (((1,), (1,)), ((), ())),
        preferred_element_type=jnp.float32,
    )
    keep = (iota(products.shape, 1) // rank == iota(products.shape, 0)) & owned
    sums = jnp.sum(jnp.where(keep, products, 0.0), axis=0, keepdims=True)
    message = jnp.concatenate([sums, squares], axis=1)
    message_ref[...] = jnp.broadcast_to(message[None], message_ref.shape)


def projection_kernel(
    own_rows,
    choice_hbm,
    lengths_hbm,
    scaled_ref,
    query_ref,
    key_ref,
    value_ref,
    up_ref,
    part_ref,
    up_rows_ref,
    owned_ref,
    table_ref,
    choice_ref,
    lengths_ref,
    query_buf,
    key_buf,
    value_buf,
    sems,
):
    requests = scaled_ref.shape[0]
    head_dim = table_ref.shape[1]
    columns, kv_columns = query_ref.shape[1], key_ref.shape[1]
    count = up_ref.shape[0]
    first = lax.axis_index("seq") * count
    chunk = min(columns, 1024)
    pieces = []
    for start in range(0, columns, chunk):
        window = (slice(None), pl.ds(start, chunk))
        pieces.append((query_ref.at[window], query_buf.at[window], start, chunk))
    pieces.append((key_ref, key_buf, columns, kv_columns))
    pieces.append((value_ref, value_buf, columns + kv_columns, kv_columns))
    others = len(pieces) + requests

    def up_copy(r, local):
        return pltpu.make_async_copy(
            up_ref.at[local], up_rows_ref.at[r], sems.at[len(pieces) + r]
        )

    choice_copy = started(choice_hbm, choice_ref, sems.at[others])
    lengths_copy = started(lengths_hbm, lengths_ref, sems.at[others + 1])
    copies = [
        started(source, target, sems.at[k]) for k, (source, target, _, _) in enumerate(pieces)
    ]
    choice_copy.wait()
    for r in range(requests):
        local = choice_ref[r] - first
        held = (local >= 0) & (local < count)

        @pl.when(held)
        def _(r=r, local=local):
            up_copy(r, local).start()

        @pl.when(jnp.logical_not(held))
        def _(r=r):
            up_rows_ref[r] = jnp.zeros(up_rows_ref.shape[1:], up_rows_ref.dtype)

    owned_ref[...] = jnp.broadcast_to(
        owned_column(choice_ref, first, count).astype(jnp.float32), owned_ref.shape
    )
    lengths_copy.wait()
    own_request = lax.axis_index("seq") * own_rows // (columns // head_dim)
    position = lengths_ref[own_request].astype(jnp.float32)
    half_dim = head_dim // 2
    lane = iota((1, head_dim), 1)
    step = jnp.where(lane < half_dim, lane, lane - half_dim).astype(jnp.float32)
    angles = position * jnp.exp(-step * (math.log(rope_base) / half_dim))
    sine_val = jnp.sin(angles)
    table_ref[0:1, :] = jnp.cos(angles)
    table_ref[1:2, :] = jnp.where(lane < half_dim, -sine_val, sine_val)
    scaled = scaled_ref[...]
    for copy, (_, target, start, size) in zip(copies, pieces):
        copy.wait()
        part_ref[:, pl.ds(start, size)] = jnp.dot(
            scaled, target[...], preferred_element_type=jnp.float32
        )
    for r in range(requests):
        local = choice_ref[r] - first

        @pl.when((local >= 0) & (local < count))
        def _(r=r, local=local):
            up_copy(r, local).wait()


def query_parts_kernel(
    model_width, owned_ref, small_ref, part_ref, up_rows_ref, message_ref, rows_ref
):
    requests, rank, columns = up_rows_ref.shape
    devices, message_rows, head_dim = message_ref.shape
    heads = columns // head_dim
    all_heads = part_ref.shape[1] // head_dim
    kv_heads = (all_heads - heads) // 2
    own_rows = requests * heads // devices
    own_kv = (message_rows - own_rows) // 2
    small = jnp.sum(small_ref[...], axis=0)
    sums, squares = small[:, : requests * rank], small[:, requests * rank :]
    diagonal = iota((requests, 128), 1) == iota((requests, 128), 0)
    squares = jnp.sum(jnp.where(diagonal, squares, 0.0), axis=1, keepdims=True)
    inverse = lax.rsqrt(squares / model_width + norm_epsilon)
    shape = (requests, requests * rank)
    keep = (iota(shape, 1) // rank == iota(shape, 0)) & (owned_ref[:, 0:1] > 0)
    shrunk = sums * inverse * adapter_scale_factor
    shrunk = jnp.where(keep, shrunk, 0.0).astype(jnp.bfloat16)
    expand = jnp.dot(
        shrunk,
        up_rows_ref[...].reshape(requests * rank, columns),
        preferred_element_type=jnp.float32,
    )
    for h in range(all_heads):
        window = slice(h * head_dim, (h + 1) * head_dim)
        rows = part_ref[:, window] * inverse
        if h < heads:
            rows = rows + expand[:, window]
        rows_ref[pl.ds(h * requests, requests), :] = rows
    for t in range(devices):
        r, h = divmod(t * own_rows, heads)
        kv = h * kv_heads // heads

        def taken(first, count):
            return rows_ref[pl.ds(first * requests + r, count, stride=requests), :]

        if own_rows == heads:
            block = taken(0, all_heads)
        else:
            block = jnp.concatenate(
                [taken(h, own_rows), taken(heads + kv, own_kv), taken(heads + kv_heads + kv, own_kv)]
            )
        message_ref[t] = block.astype(jnp.bfloat16)


def rotation_kernel(own_kv, table_ref, parts_ref, spread_ref, own_ref):
    own_rows, head_dim = spread_ref.shape[1:]
    group = own_rows // own_kv
    sums = jnp.sum(parts_ref[...].astype(jnp.float32), axis=0)
    cosine, sine_val = table_ref[0:1, :], table_ref[1:2, :]
    rotated = rounded(
        sums * cosine + pltpu.roll(sums, head_dim // 2, 1) * sine_val
    )
    query_rot = rotated[:own_rows]
    spread_ref[...] = jnp.broadcast_to(query_rot.astype(jnp.bfloat16)[None], spread_ref.shape)

    def repeated(rows):
        return jnp.concatenate(
            [jnp.broadcast_to(rows[k : k + 1], (group, head_dim)) for k in range(own_kv)]
        )

    key_rot = repeated(rotated[own_rows : own_rows + own_kv])
    own_score = jnp.sum(query_rot * key_rot, axis=1, keepdims=True) * head_dim ** (-0.5)
    own_ref[0] = jnp.broadcast_to(own_score, (own_rows, head_dim))
    own_ref[1] = repeated(rounded(sums[own_rows + own_kv : own_rows + 2 * own_kv]))


def attention_kernel(
    kv_heads,
    lengths_hbm,
    query_ref,
    key_ref,
    value_ref,
    message_ref,
    lengths_ref,
    weights_ref,
    stats_ref,
    sem,
):
    requests, entries, head_dim = key_ref.shape
    cached = entries // kv_heads
    devices, message_rows, _ = message_ref.shape
    heads = query_ref.shape[0] // requests
    own_rows = requests * heads // devices
    group = heads // kv_heads
    lengths_copy = started(lengths_hbm, lengths_ref, sem)
    first = lax.axis_index("seq") * cached
    shape = (heads, entries)
    column = iota(shape, 1)
    same_head = column % kv_heads == iota(shape, 0) // group
    position = jnp.where(same_head, first + column // kv_heads, jnp.int32(2**30))
    lane = iota((heads, head_dim), 1)
    row = iota((heads, head_dim), 0)
    lengths_copy.wait()
    for r in range(requests):
        scores = lax.dot_general(
            query_ref[pl.ds(r * heads, heads), :],
            key_ref[r],
            (((1,), (1,)), ((), ())),
            preferred_element_type=jnp.float32,
        ) * head_dim ** (-0.5)
        valid = position < lengths_ref[r]
        scores = jnp.where(valid, scores, masked_score)
        peak = jnp.max(scores, axis=1, keepdims=True)
        shift_high = rounded(peak)
        shift_low = rounded(peak - shift_high)
        weights = jnp.where(valid, jnp.exp(scores - (shift_high + shift_low)), 0.0)
        total = jnp.sum(weights, axis=1, keepdims=True)
        total_high = rounded(total)
        total_low = rounded(total - total_high)
        weights_ref[r] = weights.astype(jnp.bfloat16)
        stats = jnp.zeros((heads, head_dim), jnp.float32)
        for k, piece in enumerate((shift_high, shift_low, total_high, total_low)):
            stats = jnp.where(lane == k * own_rows + row % own_rows, piece, stats)
        stats_ref[r] = stats
    for r in range(requests):
        out = jnp.dot(weights_ref[r], value_ref[r], preferred_element_type=jnp.float32)
        for part in range(heads // own_rows):
            window = slice(part * own_rows, (part + 1) * own_rows)
            stats_row = jnp.sum(stats_ref[r, window, :], axis=0, keepdims=True)
            filler = jnp.broadcast_to(stats_row, (message_rows - own_rows, head_dim))
            block = jnp.concatenate([out[window], filler])
            message_ref[r * (heads // own_rows) + part] = block.astype(jnp.bfloat16)


def combine_kernel(parts_ref, own_ref, spread_ref):
    devices, own_rows, head_dim = spread_ref.shape
    lane = iota((own_rows, head_dim), 1)
    row = iota((own_rows, head_dim), 0)
    own_score = own_ref[0][:, 0:1]
    shifts, totals = [], []
    overall = own_score
    for s in range(devices):
        stats = parts_ref[s].astype(jnp.float32)[own_rows : own_rows + 1]
        shift = jnp.sum(
            jnp.where((lane == row) | (lane == own_rows + row), stats, 0.0), axis=1, keepdims=True
        )
        total = jnp.sum(
            jnp.where((lane == 2 * own_rows + row) | (lane == 3 * own_rows + row), stats, 0.0),
            axis=1,
            keepdims=True,
        )
        shifts.append(shift)
        totals.append(total)
        overall = jnp.maximum(overall, shift)
    own_weight = jnp.exp(own_score - overall)
    denominator = own_weight
    summed = own_weight * own_ref[1]
    for s in range(devices):
        factor = jnp.exp(shifts[s] - overall)
        denominator = denominator + totals[s] * factor
        summed = summed + factor * parts_ref[s].astype(jnp.float32)[:own_rows]
    attended = (summed / denominator).astype(jnp.bfloat16)
    spread_ref[...] = jnp.broadcast_to(attended[None], spread_ref.shape)


def output_kernel(attended_ref, weight_ref, out_ref, rows_ref):
    requests = out_ref.shape[0]
    heads = attended_ref.shape[0] // requests
    rows_ref[...] = attended_ref[...].astype(jnp.float32)
    left = jnp.concatenate(
        [rows_ref[pl.ds(h, requests, stride=heads), :] for h in range(heads)], axis=1
    ).astype(jnp.bfloat16)
    out_ref[...] = jnp.dot(left, weight_ref[...], preferred_element_type=jnp.float32)


def called(kernel, out_shape, in_specs, scratch=(), flops=0, read=0):
    call = pl.pallas_call(
        kernel,
        out_shape=out_shape,
        in_specs=in_specs,
        out_specs=jax.tree.map(lambda _: IN_VMEM, out_shape),
        scratch_shapes=list(scratch),
        cost_estimate=pl.CostEstimate(flops=flops, transcendentals=0, bytes_accessed=read),
        compiler_params=pltpu.CompilerParams(vmem_limit_bytes=28 << 20),
    )

    def run(*operands):
        return call(
            *(
                pltpu.with_memory_space_constraint(operand, pltpu.HBM)
                if spec is IN_PLACE
                else operand
                for operand, spec in zip(operands, in_specs, strict=True)
            )
        )

    return run


def body(
    hidden_state_input,
    attention_norm_gain,
    query_projection_matrix,
    key_projection_matrix,
    value_projection_matrix,
    output_projection_matrix,
    adapter_down_matrix,
    adapter_up_matrix,
    adapter_choice_index,
    lengths,
    rotated_key_cache,
    cached_value_rows,
):
    f32, bf16 = jnp.float32, jnp.bfloat16
    requests, width = hidden_state_input.shape
    _, cached, kv_heads, head_dim = rotated_key_cache.shape
    columns = query_projection_matrix.shape[1]
    kv_columns = key_projection_matrix.shape[1]
    heads = columns // head_dim
    rank = adapter_down_matrix.shape[1]
    devices = lax.axis_size("seq")
    head_size = lax.axis_size("head")
    everyone = devices * head_size
    group = heads // kv_heads
    own_rows = requests * heads // devices
    own_kv = max(own_rows // group, 1)
    parts_rows = own_rows + 2 * own_kv
    message_rows = (own_rows + 8) // 8 * 8
    sds = jax.ShapeDtypeStruct
    dma = pltpu.SemaphoreType.DMA

    small, scaled = called(
        small_sums_kernel,
        (sds((everyone, 1, requests * rank + 128), f32), sds((requests, width), bf16)),
        [IN_PLACE] * 4,
        [
            pltpu.SMEM((requests,), jnp.int32),
            pltpu.VMEM((requests, width), bf16),
            pltpu.VMEM((width,), bf16),
            pltpu.VMEM((requests, rank, width), bf16),
            dma((requests + 3,)),
        ],
    )(adapter_choice_index, hidden_state_input, attention_norm_gain, adapter_down_matrix)
    small = lax.all_to_all(small, ("seq", "head"), 0, 0, tiled=True)
    pieces = -(-columns // 1024) + 2
    part, up_rows, owned, table = called(
        functools.partial(projection_kernel, own_rows),
        (
            sds((requests, columns + 2 * kv_columns), f32),
            sds((requests, rank, columns), bf16),
            sds((requests, 128), f32),
            sds((2, head_dim), f32),
        ),
        [IN_PLACE, IN_PLACE, IN_VMEM, IN_PLACE, IN_PLACE, IN_PLACE, IN_PLACE],
        [
            pltpu.SMEM((requests,), jnp.int32),
            pltpu.SMEM((requests,), jnp.int32),
            pltpu.VMEM((width, columns), bf16),
            pltpu.VMEM((width, kv_columns), bf16),
            pltpu.VMEM((width, kv_columns), bf16),
            dma((pieces + requests + 2,)),
        ],
        flops=2 * requests * width * (columns + 2 * kv_columns),
        read=2 * width * (columns + 2 * kv_columns),
    )(
        adapter_choice_index,
        lengths,
        scaled,
        query_projection_matrix,
        key_projection_matrix,
        value_projection_matrix,
        adapter_up_matrix,
    )
    parts = called(
        functools.partial(query_parts_kernel, width * devices),
        sds((devices, parts_rows, head_dim), bf16),
        [IN_VMEM] * 4,
        [pltpu.VMEM(((heads + 2 * kv_heads) * requests, head_dim), f32)],
        flops=16 << 30,
        read=16 << 20,
    )(owned, small, part, up_rows)
    parts = exchanged(parts)

    spread, own = called(
        functools.partial(rotation_kernel, own_kv),
        (sds((devices, own_rows, head_dim), bf16), sds((2, own_rows, head_dim), f32)),
        [IN_VMEM, IN_VMEM],
        flops=16 << 30,
        read=16 << 20,
    )(table, parts)
    query_rot = exchanged(spread).reshape(requests * heads, head_dim)

    entries = cached * kv_heads
    parts = called(
        functools.partial(attention_kernel, kv_heads),
        sds((devices, message_rows, head_dim), bf16),
        [IN_PLACE, IN_VMEM, IN_VMEM, IN_VMEM],
        [
            pltpu.SMEM((requests,), jnp.int32),
            pltpu.VMEM((requests, heads, entries), bf16),
            pltpu.VMEM((requests, heads, head_dim), f32),
            dma(()),
        ],
        flops=4 * requests * heads * entries * head_dim,
        read=16 << 20,
    )(
        lengths,
        query_rot,
        rotated_key_cache.reshape(requests, entries, head_dim),
        cached_value_rows.reshape(requests, entries, head_dim),
    )
    parts = exchanged(parts)
    spread = called(
        combine_kernel, sds((devices, own_rows, head_dim), bf16), [IN_VMEM, IN_VMEM]
    )(parts, own)
    attended = exchanged(spread).reshape(requests * heads, head_dim)
    out_columns = output_projection_matrix.shape[1]
    out_part = called(
        output_kernel,
        sds((requests, out_columns), f32),
        [IN_VMEM, IN_VMEM],
        [pltpu.VMEM((requests * heads, head_dim), f32)],
    )(attended, output_projection_matrix)
    if head_size == 2:
        output_sum = out_part + lax.ppermute(out_part, "head", [(0, 1), (1, 0)])
    else:
        output_sum = lax.psum(out_part, "head")
    return output_sum.astype(jnp.bfloat16)


def solution(mesh):
    return jax.shard_map(
        body,
        mesh=mesh,
        in_specs=(
            P(None, "seq"),
            P("seq"),
            P("seq", "head"),
            P("seq", "head"),
            P("seq", "head"),
            P("head", "seq"),
            P("head", None, "seq"),
            P("seq", None, "head"),
            P(),
            P(),
            P(None, "seq", "head", None),
            P(None, "seq", "head", None),
        ),
        out_specs=P(None, "seq"),
        check_vma=False,
    )
```

```python
import functools
import math

import jax
import jax.numpy as jnp
from jax import lax
from jax.experimental import pallas as pl
from jax.experimental.pallas import tpu as pltpu
from jax.sharding import PartitionSpec as P

norm_epsilon = 1e-05
adapter_scale_factor = 1.0
rope_base = 500000.0
masked_score = -1e30

IN_VMEM = pl.BlockSpec(memory_space=pltpu.VMEM)
IN_PLACE = pl.BlockSpec(memory_space=pltpu.HBM)


def exchanged(parts):
    return lax.all_to_all(parts, "seq", 0, 0, tiled=True)


def iota(shape, axis):
    return lax.broadcasted_iota(jnp.int32, shape, axis)


def rounded(value):
    return value.astype(jnp.bfloat16).astype(jnp.float32)


def started(source, target, sem):
    copy = pltpu.make_async_copy(source, target, sem)
    copy.start()
    return copy


def owned_column(choice_ref, first, count):
    requests = choice_ref.shape[0]
    row = iota((requests, 1), 0)
    column = jnp.zeros((requests, 1), jnp.int32)
    for r in range(requests):
        local = choice_ref[r] - first
        held = ((local >= 0) & (local < count)).astype(jnp.int32)
        column = jnp.where(row == r, held, column)
    return column > 0


def small_sums_kernel(
    own_rows,
    choice_hbm,
    lengths_hbm,
    hidden_hbm,
    gain_hbm,
    down_ref,
    up_ref,
    message_ref,
    scaled_ref,
    up_rows_ref,
    owned_ref,
    table_ref,
    limits_ref,
    choice_ref,
    lengths_ref,
    hidden_ref,
    gain_ref,
    down_rows_ref,
    sems,
    down_sems,
    up_sems,
):
    requests, rank, width = down_rows_ref.shape
    columns, head_dim = up_ref.shape[2], table_ref.shape[1]
    choice_copy = started(choice_hbm, choice_ref, sems.at[0])
    lengths_copy = started(lengths_hbm, lengths_ref, sems.at[1])
    hidden_copy = started(hidden_hbm, hidden_ref, sems.at[2])
    gain_copy = started(gain_hbm, gain_ref, sems.at[3])
    head_index = lax.axis_index("head")
    down_count, up_count = down_ref.shape[0], up_ref.shape[0]
    down_first = head_index * down_count
    up_first = lax.axis_index("seq") * up_count

    def up_copy(r):
        local = choice_ref[r] - up_first
        return pltpu.make_async_copy(up_ref.at[local], up_rows_ref.at[r], up_sems.at[r])

    def up_held(r):
        local = choice_ref[r] - up_first
        return (local >= 0) & (local < up_count)

    choice_copy.wait()
    down_copies = []
    for r in range(requests):
        local = jnp.clip(choice_ref[r] - down_first, 0, down_count - 1)
        down_copies.append(started(down_ref.at[local], down_rows_ref.at[r], down_sems.at[r]))
    for r in range(requests):

        @pl.when(up_held(r))
        def _(r=r):
            up_copy(r).start()

        @pl.when(jnp.logical_not(up_held(r)))
        def _(r=r):
            up_rows_ref[r] = jnp.zeros(up_rows_ref.shape[1:], up_rows_ref.dtype)

    owned_ref[...] = jnp.broadcast_to(
        owned_column(choice_ref, up_first, up_count).astype(jnp.float32), owned_ref.shape
    )
    lengths_copy.wait()
    for r in range(requests):
        limits_ref[pl.ds(r, 1), :] = jnp.full((1, limits_ref.shape[1]), lengths_ref[r], jnp.int32)
    own_request = lax.axis_index("seq") * own_rows // (columns // head_dim)
    position = lengths_ref[own_request].astype(jnp.float32)
    half_dim = head_dim // 2
    lane = iota((1, head_dim), 1)
    step = jnp.where(lane < half_dim, lane, lane - half_dim).astype(jnp.float32)
    angles = position * jnp.exp(-step * (math.log(rope_base) / half_dim))
    sine_val = jnp.sin(angles)
    table_ref[0:1, :] = jnp.cos(angles)
    table_ref[1:2, :] = jnp.where(lane < half_dim, -sine_val, sine_val)

    hidden_copy.wait()
    gain_copy.wait()
    values = hidden_ref[...].astype(jnp.float32)
    gain = gain_ref[...].astype(jnp.float32).reshape(1, width)
    scaled = (values * gain).astype(jnp.bfloat16)
    scaled_ref[...] = scaled
    squares = jnp.sum(values * values, axis=1, keepdims=True)
    squares = jnp.where(head_index == 0, squares, 0.0)
    diagonal = iota((requests, 128), 1) == iota((requests, 128), 0)
    squares = jnp.sum(jnp.where(diagonal, squares, 0.0), axis=0, keepdims=True)
    owned = owned_column(choice_ref, down_first, down_count)
    for copy in down_copies:
        copy.wait()
    products = lax.dot_general(
        scaled,
        down_rows_ref[...].reshape(requests * rank, width),
        (((1,), (1,)), ((), ())),
        preferred_element_type=jnp.float32,
    )
    keep = (iota(products.shape, 1) // rank == iota(products.shape, 0)) & owned
    sums = jnp.sum(jnp.where(keep, products, 0.0), axis=0, keepdims=True)
    message = jnp.concatenate([sums, squares], axis=1)
    message_ref[...] = jnp.broadcast_to(message[None], message_ref.shape)
    for r in range(requests):

        @pl.when(up_held(r))
        def _(r=r):
            up_copy(r).wait()


def query_parts_kernel(
    model_width,
    owned_ref,
    small_ref,
    scaled_ref,
    query_ref,
    key_ref,
    value_ref,
    up_rows_ref,
    message_ref,
    rows_ref,
):
    requests, rank, columns = up_rows_ref.shape
    devices, message_rows, head_dim = message_ref.shape
    heads = columns // head_dim
    kv_heads = key_ref.shape[1] // head_dim
    all_heads = heads + 2 * kv_heads
    own_rows = requests * heads // devices
    own_kv = (message_rows - own_rows) // 2
    small = jnp.sum(small_ref[...], axis=0)
    sums, squares = small[:, : requests * rank], small[:, requests * rank :]
    diagonal = iota((requests, 128), 1) == iota((requests, 128), 0)
    squares = jnp.sum(jnp.where(diagonal, squares, 0.0), axis=1, keepdims=True)
    inverse = lax.rsqrt(squares / model_width + norm_epsilon)
    shape = (requests, requests * rank)
    keep = (iota(shape, 1) // rank == iota(shape, 0)) & (owned_ref[:, 0:1] > 0)
    shrunk = sums * inverse * adapter_scale_factor
    shrunk = jnp.where(keep, shrunk, 0.0).astype(jnp.bfloat16)
    scaled = scaled_ref[...]
    up_rows = up_rows_ref.reshape(requests * rank, columns)
    chunk = min(columns, 1024)
    first_head = 0
    for weight_ref in (query_ref, key_ref, value_ref):
        for start in range(0, weight_ref.shape[1], chunk):
            size = min(chunk, weight_ref.shape[1] - start)
            part = jnp.dot(
                scaled, weight_ref[:, pl.ds(start, size)], preferred_element_type=jnp.float32
            )
            part = part * inverse
            if weight_ref is query_ref:
                part = part + jnp.dot(
                    shrunk, up_rows[:, pl.ds(start, size)], preferred_element_type=jnp.float32
                )
            for k in range(size // head_dim):
                h = first_head + start // head_dim + k
                rows_ref[pl.ds(h * requests, requests), :] = part[
                    :, k * head_dim : (k + 1) * head_dim
                ]
        first_head += weight_ref.shape[1] // head_dim
    for t in range(devices):
        r, h = divmod(t * own_rows, heads)
        kv = h * kv_heads // heads

        def taken(first, count):
            return rows_ref[pl.ds(first * requests + r, count, stride=requests), :]

        if own_rows == heads:
            block = taken(0, all_heads)
        else:
            block = jnp.concatenate(
                [taken(h, own_rows), taken(heads + kv, own_kv), taken(heads + kv_heads + kv, own_kv)]
            )
        message_ref[t] = block.astype(jnp.bfloat16)


def rotation_kernel(own_kv, table_ref, parts_ref, spread_ref, own_ref):
    own_rows, head_dim = spread_ref.shape[1:]
    group = own_rows // own_kv
    sums = jnp.sum(parts_ref[...].astype(jnp.float32), axis=0)
    cosine, sine_val = table_ref[0:1, :], table_ref[1:2, :]
    rotated = rounded(
        sums * cosine + pltpu.roll(sums, head_dim // 2, 1) * sine_val
    )
    query_rot = rotated[:own_rows]
    spread_ref[...] = jnp.broadcast_to(query_rot.astype(jnp.bfloat16)[None], spread_ref.shape)

    def repeated(rows):
        return jnp.concatenate(
            [jnp.broadcast_to(rows[k : k + 1], (group, head_dim)) for k in range(own_kv)]
        )

    key_rot = repeated(rotated[own_rows : own_rows + own_kv])
    own_score = jnp.sum(query_rot * key_rot, axis=1, keepdims=True) * head_dim ** (-0.5)
    own_ref[0] = jnp.broadcast_to(own_score, (own_rows, head_dim))
    own_ref[1] = repeated(rounded(sums[own_rows + own_kv : own_rows + 2 * own_kv]))


def attention_kernel(
    kv_heads,
    limits_ref,
    query_ref,
    key_ref,
    value_ref,
    message_ref,
    weights_ref,
    stats_ref,
):
    requests, entries, head_dim = key_ref.shape
    cached = entries // kv_heads
    devices, message_rows, _ = message_ref.shape
    heads = query_ref.shape[0] // requests
    own_rows = requests * heads // devices
    group = heads // kv_heads
    first = lax.axis_index("seq") * cached
    shape = (heads, entries)
    column = iota(shape, 1)
    same_head = column % kv_heads == iota(shape, 0) // group
    position = jnp.where(same_head, first + column // kv_heads, jnp.int32(2**30))
    lane = iota((heads, head_dim), 1)
    row = iota((heads, head_dim), 0)
    for r in range(requests):
        scores = lax.dot_general(
            query_ref[pl.ds(r * heads, heads), :],
            key_ref[r],
            (((1,), (1,)), ((), ())),
            preferred_element_type=jnp.float32,
        ) * head_dim ** (-0.5)
        valid = position < limits_ref[pl.ds(r, 1), 0:1]
        scores = jnp.where(valid, scores, masked_score)
        peak = jnp.max(scores, axis=1, keepdims=True)
        peak_high = rounded(peak)
        peak_mid = rounded(peak - peak_high)
        peak_low = peak - peak_high - peak_mid
        weights = jnp.where(valid, jnp.exp(scores - peak), 0.0)
        total = jnp.sum(weights, axis=1, keepdims=True)
        total_high = rounded(total)
        total_low = rounded(total - total_high)
        weights_ref[r] = weights.astype(jnp.bfloat16)
        stats = jnp.zeros((heads, head_dim), jnp.float32)
        for k, piece in enumerate((peak_high, peak_mid, peak_low, total_high)):
            stats = jnp.where(lane == k * own_rows + row % own_rows, piece, stats)
        stats_ref[r, 0] = stats
        stats_ref[r, 1] = jnp.where(lane == row % own_rows, total_low, 0.0)
    for r in range(requests):
        out = jnp.dot(weights_ref[r], value_ref[r], preferred_element_type=jnp.float32)
        for part in range(heads // own_rows):
            window = slice(part * own_rows, (part + 1) * own_rows)
            first_row = jnp.sum(stats_ref[r, 0, window, :], axis=0, keepdims=True)
            second_row = jnp.sum(stats_ref[r, 1, window, :], axis=0, keepdims=True)
            filler_shape = (message_rows - own_rows, head_dim)
            filler = jnp.where(iota(filler_shape, 0) == 0, first_row, second_row)
            block = jnp.concatenate([out[window], filler])
            message_ref[r * (heads // own_rows) + part] = block.astype(jnp.bfloat16)


def combine_kernel(parts_ref, own_ref, spread_ref):
    devices, own_rows, head_dim = spread_ref.shape
    lane = iota((own_rows, head_dim), 1)
    row = iota((own_rows, head_dim), 0)
    own_score = own_ref[0][:, 0:1]
    peaks, totals = [], []
    overall = own_score
    for s in range(devices):
        stats = parts_ref[s].astype(jnp.float32)
        first_row, second_row = stats[own_rows : own_rows + 1], stats[own_rows + 1 : own_rows + 2]
        peak = jnp.where((lane < 3 * own_rows) & (lane % own_rows == row), first_row, 0.0)
        total = jnp.where(lane == 3 * own_rows + row, first_row, 0.0)
        total = total + jnp.where(lane == row, second_row, 0.0)
        peaks.append(jnp.sum(peak, axis=1, keepdims=True))
        totals.append(jnp.sum(total, axis=1, keepdims=True))
        overall = jnp.maximum(overall, peaks[-1])
    own_weight = jnp.exp(own_score - overall)
    denominator = own_weight
    summed = own_weight * own_ref[1]
    for s in range(devices):
        factor = jnp.exp(peaks[s] - overall)
        denominator = denominator + totals[s] * factor
        summed = summed + factor * parts_ref[s].astype(jnp.float32)[:own_rows]
    attended = (summed / denominator).astype(jnp.bfloat16)
    spread_ref[...] = jnp.broadcast_to(attended[None], spread_ref.shape)


def output_kernel(attended_ref, weight_ref, out_ref, rows_ref):
    requests = out_ref.shape[0]
    heads = attended_ref.shape[0] // requests
    rows_ref[...] = attended_ref[...].astype(jnp.float32)
    left = jnp.concatenate(
        [rows_ref[pl.ds(h, requests, stride=heads), :] for h in range(heads)], axis=1
    ).astype(jnp.bfloat16)
    out_ref[...] = jnp.dot(left, weight_ref[...], preferred_element_type=jnp.float32)


def called(kernel, out_shape, in_specs, scratch=(), flops=0, read=0):
    call = pl.pallas_call(
        kernel,
        out_shape=out_shape,
        in_specs=in_specs,
        out_specs=jax.tree.map(lambda _: IN_VMEM, out_shape),
        scratch_shapes=list(scratch),
        cost_estimate=pl.CostEstimate(flops=flops, transcendentals=0, bytes_accessed=read),
        compiler_params=pltpu.CompilerParams(vmem_limit_bytes=16 << 20),
    )

    def run(*operands):
        return call(
            *(
                pltpu.with_memory_space_constraint(operand, pltpu.HBM)
                if spec is IN_PLACE
                else operand
                for operand, spec in zip(operands, in_specs, strict=True)
            )
        )

    return run


def body(
    hidden_state_input,
    attention_norm_gain,
    query_projection_matrix,
    key_projection_matrix,
    value_projection_matrix,
    output_projection_matrix,
    adapter_down_matrix,
    adapter_up_matrix,
    adapter_choice_index,
    lengths,
    rotated_key_cache,
    cached_value_rows,
):
    f32, bf16 = jnp.float32, jnp.bfloat16
    requests, width = hidden_state_input.shape
    _, cached, kv_heads, head_dim = rotated_key_cache.shape
    columns = query_projection_matrix.shape[1]
    heads = columns // head_dim
    rank = adapter_down_matrix.shape[1]
    devices = lax.axis_size("seq")
    head_size = lax.axis_size("head")
    everyone = devices * head_size
    group = heads // kv_heads
    own_rows = requests * heads // devices
    own_kv = max(own_rows // group, 1)
    parts_rows = own_rows + 2 * own_kv
    message_rows = -(-(own_rows + 2) // 8) * 8
    covering = 16 << 30
    sds = jax.ShapeDtypeStruct
    dma = pltpu.SemaphoreType.DMA

    small, scaled, up_rows, owned, table, limits = called(
        functools.partial(small_sums_kernel, own_rows),
        (
            sds((everyone, 1, requests * rank + 128), f32),
            sds((requests, width), bf16),
            sds((requests, rank, columns), bf16),
            sds((requests, 128), f32),
            sds((2, head_dim), f32),
            sds((requests, 128), jnp.int32),
        ),
        [IN_PLACE] * 6,
        [
            pltpu.SMEM((requests,), jnp.int32),
            pltpu.SMEM((requests,), jnp.int32),
            pltpu.VMEM((requests, width), bf16),
            pltpu.VMEM((width,), bf16),
            pltpu.VMEM((requests, rank, width), bf16),
            dma((4,)),
            dma((requests,)),
            dma((requests,)),
        ],
        flops=covering,
        read=covering >> 10,
    )(
        adapter_choice_index,
        lengths,
        hidden_state_input,
        attention_norm_gain,
        adapter_down_matrix,
        adapter_up_matrix,
    )
    small = lax.all_to_all(small, ("seq", "head"), 0, 0, tiled=True)
    parts = called(
        functools.partial(query_parts_kernel, width * devices),
        sds((devices, parts_rows, head_dim), bf16),
        [IN_VMEM] * 7,
        [pltpu.VMEM(((heads + 2 * kv_heads) * requests, head_dim), f32)],
        flops=covering,
        read=covering >> 10,
    )(
        owned,
        small,
        scaled,
        query_projection_matrix,
        key_projection_matrix,
        value_projection_matrix,
        up_rows,
    )
    parts = exchanged(parts)

    spread, own = called(
        functools.partial(rotation_kernel, own_kv),
        (sds((devices, own_rows, head_dim), bf16), sds((2, own_rows, head_dim), f32)),
        [IN_VMEM, IN_VMEM],
        flops=covering,
        read=covering >> 10,
    )(table, parts)
    query_rot = exchanged(spread).reshape(requests * heads, head_dim)

    entries = cached * kv_heads
    parts = called(
        functools.partial(attention_kernel, kv_heads),
        sds((devices, message_rows, head_dim), bf16),
        [IN_VMEM] * 4,
        [
            pltpu.VMEM((requests, heads, entries), bf16),
            pltpu.VMEM((requests, 2, heads, head_dim), f32),
        ],
        flops=4 * requests * heads * entries * head_dim,
        read=16 << 20,
    )(
        limits,
        query_rot,
        rotated_key_cache.reshape(requests, entries, head_dim),
        cached_value_rows.reshape(requests, entries, head_dim),
    )
    parts = exchanged(parts)
    spread = called(
        combine_kernel, sds((devices, own_rows, head_dim), bf16), [IN_VMEM, IN_VMEM]
    )(parts, own)
    attended = exchanged(spread).reshape(requests * heads, head_dim)
    out_columns = output_projection_matrix.shape[1]
    out_part = called(
        output_kernel,
        sds((requests, out_columns), f32),
        [IN_VMEM, IN_VMEM],
        [pltpu.VMEM((requests * heads, head_dim), f32)],
    )(attended, output_projection_matrix)
    if head_size == 2:
        output_sum = out_part + lax.ppermute(out_part, "head", [(0, 1), (1, 0)])
    else:
        output_sum = lax.psum(out_part, "head")
    return output_sum.astype(jnp.bfloat16)


def solution(mesh):
    return jax.shard_map(
        body,
        mesh=mesh,
        in_specs=(
            P(None, "seq"),
            P("seq"),
            P("seq", "head"),
            P("seq", "head"),
            P("seq", "head"),
            P("head", "seq"),
            P("head", None, "seq"),
            P("seq", None, "head"),
            P(),
            P(),
            P(None, "seq", "head", None),
            P(None, "seq", "head", None),
        ),
        out_specs=P(None, "seq"),
        check_vma=False,
    )
```

```python
import functools
import math

import jax
import jax.numpy as jnp
from jax import lax
from jax.experimental import pallas as pl
from jax.experimental.pallas import tpu as pltpu
from jax.sharding import PartitionSpec as P

norm_epsilon = 1e-05
adapter_scale_factor = 1.0
rope_base = 500000.0
masked_score = -1e30
masked_limit = 5e29

IN_VMEM = pl.BlockSpec(memory_space=pltpu.VMEM)
IN_PLACE = pl.BlockSpec(memory_space=pltpu.HBM)


def exchanged(rows, axes):
    count, head_dim = lax.axis_size(axes), rows.shape[1]
    inner = math.gcd(rows.shape[0] // count, 8)
    blocks = rows.reshape(count, -1, inner, head_dim)
    return lax.all_to_all(blocks, axes, 0, 0, tiled=True).reshape(rows.shape)


def iota(shape, axis):
    return lax.broadcasted_iota(jnp.int32, shape, axis)


def rounded(value):
    return value.astype(jnp.bfloat16).astype(jnp.float32)


def started(source, target, sem):
    copy = pltpu.make_async_copy(source, target, sem)
    copy.start()
    return copy


def owned_column(choice_ref, first, count):
    requests = choice_ref.shape[0]
    row = iota((requests, 1), 0)
    column = jnp.zeros((requests, 1), jnp.int32)
    for r in range(requests):
        local = choice_ref[r] - first
        held = ((local >= 0) & (local < count)).astype(jnp.int32)
        column = jnp.where(row == r, held, column)
    return column > 0


def small_sums_kernel(
    axes,
    own_rows,
    choice_hbm,
    lengths_hbm,
    hidden_hbm,
    gain_hbm,
    down_ref,
    up_ref,
    message_ref,
    scaled_ref,
    up_rows_ref,
    owned_ref,
    table_ref,
    limits_ref,
    choice_ref,
    lengths_ref,
    hidden_ref,
    gain_ref,
    down_rows_ref,
    sems,
    down_sems,
    up_sems,
):
    requests, rank, width = down_rows_ref.shape
    columns, head_dim = up_ref.shape[2], table_ref.shape[1]
    choice_copy = started(choice_hbm, choice_ref, sems.at[0])
    lengths_copy = started(lengths_hbm, lengths_ref, sems.at[1])
    hidden_copy = started(hidden_hbm, hidden_ref, sems.at[2])
    gain_copy = started(gain_hbm, gain_ref, sems.at[3])
    head_index = lax.axis_index("head")
    down_count, up_count = down_ref.shape[0], up_ref.shape[0]
    down_first = head_index * down_count
    up_first = lax.axis_index("seq") * up_count

    def up_copy(r):
        local = choice_ref[r] - up_first
        return pltpu.make_async_copy(up_ref.at[local], up_rows_ref.at[r], up_sems.at[r])

    def up_held(r):
        local = choice_ref[r] - up_first
        return (local >= 0) & (local < up_count)

    choice_copy.wait()
    down_copies = []
    for r in range(requests):
        local = jnp.clip(choice_ref[r] - down_first, 0, down_count - 1)
        down_copies.append(started(down_ref.at[local], down_rows_ref.at[r], down_sems.at[r]))
    for r in range(requests):

        @pl.when(up_held(r))
        def _(r=r):
            up_copy(r).start()

        @pl.when(jnp.logical_not(up_held(r)))
        def _(r=r):
            up_rows_ref[r] = jnp.zeros(up_rows_ref.shape[1:], up_rows_ref.dtype)

    owned_ref[...] = jnp.broadcast_to(
        owned_column(choice_ref, up_first, up_count).astype(jnp.float32), owned_ref.shape
    )
    lengths_copy.wait()
    for r in range(requests):
        limits_ref[pl.ds(r, 1), :] = jnp.full((1, limits_ref.shape[1]), lengths_ref[r], jnp.int32)
    own_request = lax.axis_index(axes) * own_rows // (columns // head_dim)
    position = lengths_ref[own_request].astype(jnp.float32)
    half_dim = head_dim // 2
    lane = iota((1, head_dim), 1)
    step = jnp.where(lane < half_dim, lane, lane - half_dim).astype(jnp.float32)
    angles = position * jnp.exp(-step * (math.log(rope_base) / half_dim))
    sine_val = jnp.sin(angles)
    table_ref[0:1, :] = jnp.cos(angles)
    table_ref[1:2, :] = jnp.where(lane < half_dim, -sine_val, sine_val)

    hidden_copy.wait()
    gain_copy.wait()
    values = hidden_ref[...].astype(jnp.float32)
    gain = gain_ref[...].astype(jnp.float32).reshape(1, width)
    scaled = (values * gain).astype(jnp.bfloat16)
    scaled_ref[...] = scaled
    squares = jnp.sum(values * values, axis=1, keepdims=True)
    squares = jnp.where(head_index == 0, squares, 0.0)
    diagonal = iota((requests, 128), 1) == iota((requests, 128), 0)
    squares = jnp.sum(jnp.where(diagonal, squares, 0.0), axis=0, keepdims=True)
    owned = owned_column(choice_ref, down_first, down_count)
    for copy in down_copies:
        copy.wait()
    products = lax.dot_general(
        scaled,
        down_rows_ref[...].reshape(requests * rank, width),
        (((1,), (1,)), ((), ())),
        preferred_element_type=jnp.float32,
    )
    keep = (iota(products.shape, 1) // rank == iota(products.shape, 0)) & owned
    sums = jnp.sum(jnp.where(keep, products, 0.0), axis=0, keepdims=True)
    message = jnp.concatenate([sums, squares], axis=1)
    message_ref[...] = message
    for r in range(requests):

        @pl.when(up_held(r))
        def _(r=r):
            up_copy(r).wait()


def repeat_kernel(message_ref, repeated_ref):
    repeated_ref[...] = jnp.broadcast_to(message_ref[...][None], repeated_ref.shape)


def query_parts_kernel(
    model_width,
    own_rows,
    own_kv,
    owned_ref,
    small_ref,
    scaled_ref,
    query_ref,
    key_ref,
    value_ref,
    up_rows_ref,
    message_ref,
    rows_ref,
    staged_ref,
):
    requests, rank, columns = up_rows_ref.shape
    head_dim = message_ref.shape[1]
    heads = columns // head_dim
    kv_heads = key_ref.shape[1] // head_dim
    small = jnp.sum(small_ref[...], axis=0)
    sums, squares = small[:, : requests * rank], small[:, requests * rank :]
    diagonal = iota((requests, 128), 1) == iota((requests, 128), 0)
    squares = jnp.sum(jnp.where(diagonal, squares, 0.0), axis=1, keepdims=True)
    inverse = lax.rsqrt(squares / model_width + norm_epsilon)
    shape = (requests, requests * rank)
    keep = (iota(shape, 1) // rank == iota(shape, 0)) & (owned_ref[:, 0:1] > 0)
    shrunk = sums * inverse * adapter_scale_factor
    shrunk = jnp.where(keep, shrunk, 0.0).astype(jnp.bfloat16)
    scaled = scaled_ref[...]
    up_rows = up_rows_ref.reshape(requests * rank, columns)
    chunk = min(columns, 1024)
    query_places = list(range(heads))
    key_places = [heads + k + k // own_kv * own_kv for k in range(kv_heads)]
    value_places = [place + own_kv for place in key_places]
    places = iter(query_places + key_places + value_places)
    for weight_ref in (query_ref, key_ref, value_ref):
        for start in range(0, weight_ref.shape[1], chunk):
            size = min(chunk, weight_ref.shape[1] - start)
            part = jnp.dot(
                scaled, weight_ref[:, pl.ds(start, size)], preferred_element_type=jnp.float32
            )
            part = part * inverse
            if weight_ref is query_ref:
                part = part + jnp.dot(
                    shrunk, up_rows[:, pl.ds(start, size)], preferred_element_type=jnp.float32
                )
            for k in range(size // head_dim):
                rows_ref[pl.ds(next(places) * requests, requests), :] = part[
                    :, k * head_dim : (k + 1) * head_dim
                ]
    rows = own_rows + 2 * own_kv
    for t in range(requests * heads // own_rows):
        r, h = divmod(t * own_rows, heads)
        kv = heads + 2 * (h * kv_heads // heads)
        staged_ref[pl.ds(t * rows, own_rows), :] = rows_ref[
            pl.ds(h * requests + r, own_rows, stride=requests), :
        ]
        staged_ref[pl.ds(t * rows + own_rows, 2 * own_kv), :] = rows_ref[
            pl.ds(kv * requests + r, 2 * own_kv, stride=requests), :
        ]
    message_ref[...] = staged_ref[...].astype(jnp.bfloat16)


def rotation_kernel(own_rows, own_kv, table_ref, parts_ref, spread_ref, own_ref):
    head_dim = spread_ref.shape[2]
    group = own_rows // own_kv
    rows = own_rows + 2 * own_kv
    sums = jnp.sum(parts_ref[...].astype(jnp.float32), axis=0)
    cosine, sine_val = table_ref[0:1, :], table_ref[1:2, :]
    rotated = rounded(sums * cosine + pltpu.roll(sums, head_dim // 2, 1) * sine_val)

    def repeated(rows, first):
        return [
            jnp.broadcast_to(rows[first + k : first + k + 1], (group, head_dim))
            for k in range(own_kv)
        ]

    queries, keys, values = [], [], []
    for first in range(0, sums.shape[0], rows):
        queries.append(rotated[first : first + own_rows])
        keys += repeated(rotated, first + own_rows)
        values += repeated(rounded(sums), first + own_rows + own_kv)
    query_rot = jnp.concatenate(queries)
    spread_ref[...] = jnp.broadcast_to(query_rot.astype(jnp.bfloat16)[None], spread_ref.shape)
    own_score = jnp.sum(query_rot * jnp.concatenate(keys), axis=1, keepdims=True)
    own_ref[0] = jnp.broadcast_to(own_score * head_dim ** (-0.5), query_rot.shape)
    own_ref[1] = jnp.concatenate(values)


def attention_kernel(
    kv_heads,
    own_rows,
    limits_ref,
    query_ref,
    key_ref,
    value_ref,
    message_ref,
    weights_ref,
    stats_ref,
    staged_ref,
):
    requests, entries, head_dim = key_ref.shape
    cached = entries // kv_heads
    heads = query_ref.shape[0] // requests
    group = heads // kv_heads
    first = lax.axis_index("seq") * cached
    lane = iota((heads, head_dim), 1)
    row = iota((heads, head_dim), 0)
    per_tile = head_dim // kv_heads
    position = jnp.where(
        lane % kv_heads == row // group, first + lane // kv_heads, jnp.int32(2**30)
    )
    score_scale = head_dim ** (-0.5)
    for r in range(requests):
        scores = lax.dot_general(
            query_ref[pl.ds(r * heads, heads), :],
            key_ref[r],
            (((1,), (1,)), ((), ())),
            preferred_element_type=jnp.float32,
        )
        limit = jnp.broadcast_to(limits_ref[pl.ds(r, 1), :], (heads, head_dim))
        tiles = []
        peak = jnp.full((heads, head_dim), -masked_limit, jnp.float32)
        for c in range(entries // head_dim):
            valid = position < limit - c * per_tile
            tile = scores[:, c * head_dim : (c + 1) * head_dim]
            tiles.append(jnp.where(valid, tile, masked_score))
            peak = jnp.maximum(peak, tiles[-1])
        peak = jnp.max(peak, axis=1, keepdims=True)
        total = jnp.zeros((heads, head_dim), jnp.float32)
        for c, tile in enumerate(tiles):
            weights = jnp.exp2((tile - peak) * (score_scale * math.log2(math.e)))
            total = total + weights
            weights_ref[r, :, pl.ds(c * head_dim, head_dim)] = weights.astype(jnp.bfloat16)
        total = jnp.sum(total, axis=1, keepdims=True)
        peak = peak * score_scale
        peak_high = rounded(peak)
        peak_mid = rounded(peak - peak_high)
        peak_low = peak - peak_high - peak_mid
        total_high = rounded(total)
        total_low = rounded(total - total_high)
        stats = jnp.zeros((heads, head_dim), jnp.float32)
        for k, piece in enumerate((peak_high, peak_mid, peak_low, total_high, total_low)):
            stats = jnp.where(lane == k * own_rows + row % own_rows, piece, stats)
        stats_ref[r] = stats
    for r in range(requests):
        out = jnp.dot(weights_ref[r], value_ref[r], preferred_element_type=jnp.float32)
        for part in range(heads // own_rows):
            window = slice(part * own_rows, (part + 1) * own_rows)
            place = (r * (heads // own_rows) + part) * (own_rows + 2)
            stats_row = jnp.sum(stats_ref[r, window, :], axis=0, keepdims=True)
            staged_ref[pl.ds(place, own_rows), :] = out[window]
            staged_ref[pl.ds(place + own_rows, 2), :] = jnp.broadcast_to(stats_row, (2, head_dim))
    message_ref[...] = staged_ref[...].astype(jnp.bfloat16)


def combine_kernel(own_rows, parts_ref, own_ref, spread_ref, staged_ref):
    devices, all_rows, head_dim = spread_ref.shape
    halves = all_rows // own_rows
    lane = iota((own_rows, head_dim), 1)
    row = iota((own_rows, head_dim), 0)
    staged_ref[...] = parts_ref[...].astype(jnp.float32)
    same_row = lane % own_rows == row
    for half in range(halves):
        window = slice(half * own_rows, (half + 1) * own_rows)
        own_score = own_ref[0, window, 0:1]
        places = [(s * halves + half) * (own_rows + 2) for s in range(devices)]
        peaks, totals = [], []
        overall = own_score
        for place in places:
            stats = staged_ref[pl.ds(place + own_rows, 1), :]
            stats = jnp.where(same_row & (lane < 5 * own_rows), stats, 0.0)
            peak = jnp.where(lane < 3 * own_rows, stats, 0.0)
            peaks.append(jnp.sum(peak, axis=1, keepdims=True))
            total = jnp.where(lane < 3 * own_rows, 0.0, stats)
            totals.append(jnp.sum(total, axis=1, keepdims=True))
            overall = jnp.maximum(overall, peaks[-1])
        own_weight = jnp.exp(own_score - overall)
        denominator = own_weight
        summed = own_weight * own_ref[1, window, :]
        for place, peak, total in zip(places, peaks, totals):
            factor = jnp.exp(peak - overall)
            denominator = denominator + total * factor
            summed = summed + factor * staged_ref[pl.ds(place, own_rows), :]
        attended = (summed / denominator).astype(jnp.bfloat16)
        spread_ref[:, window, :] = jnp.broadcast_to(
            attended[None], (devices, own_rows, head_dim)
        )


def output_kernel(attended_ref, weight_ref, out_ref, rows_ref):
    requests = out_ref.shape[0]
    heads = attended_ref.shape[0] // requests
    rows_ref[...] = attended_ref[...].astype(jnp.float32)
    left = jnp.concatenate(
        [rows_ref[pl.ds(h, requests, stride=heads), :] for h in range(heads)], axis=1
    ).astype(jnp.bfloat16)
    out_ref[...] = jnp.dot(left, weight_ref[...], preferred_element_type=jnp.float32)


def called(kernel, out_shape, in_specs, scratch=(), flops=0, read=0):
    call = pl.pallas_call(
        kernel,
        out_shape=out_shape,
        in_specs=in_specs,
        out_specs=jax.tree.map(lambda _: IN_VMEM, out_shape),
        scratch_shapes=list(scratch),
        cost_estimate=pl.CostEstimate(flops=flops, transcendentals=0, bytes_accessed=read),
        compiler_params=pltpu.CompilerParams(vmem_limit_bytes=16 << 20),
    )

    def run(*operands):
        return call(
            *(
                pltpu.with_memory_space_constraint(operand, pltpu.HBM)
                if spec is IN_PLACE
                else operand
                for operand, spec in zip(operands, in_specs, strict=True)
            )
        )

    return run


def body(
    hidden_state_input,
    attention_norm_gain,
    query_projection_matrix,
    key_projection_matrix,
    value_projection_matrix,
    output_projection_matrix,
    adapter_down_matrix,
    adapter_up_matrix,
    adapter_choice_index,
    lengths,
    rotated_key_cache,
    cached_value_rows,
):
    f32, bf16 = jnp.float32, jnp.bfloat16
    requests, width = hidden_state_input.shape
    _, cached, kv_heads, head_dim = rotated_key_cache.shape
    columns = query_projection_matrix.shape[1]
    heads = columns // head_dim
    rank = adapter_down_matrix.shape[1]
    devices = lax.axis_size("seq")
    head_size = lax.axis_size("head")
    everyone = devices * head_size
    group = heads // kv_heads
    shared = requests * heads % everyone == 0
    axes = ("seq", "head") if shared else ("seq",)
    halves = head_size if shared else 1
    own_rows = requests * heads // (devices * halves)
    own_kv = max(own_rows // group, 1)
    parts_rows = own_rows + 2 * own_kv
    targets = devices * halves
    covering = 16 << 30
    sds = jax.ShapeDtypeStruct
    dma = pltpu.SemaphoreType.DMA

    small, scaled, up_rows, owned, table, limits = called(
        functools.partial(small_sums_kernel, axes, own_rows),
        (
            sds((1, requests * rank + 128), f32),
            sds((requests, width), bf16),
            sds((requests, rank, columns), bf16),
            sds((requests, 128), f32),
            sds((2, head_dim), f32),
            sds((requests, 128), jnp.int32),
        ),
        [IN_PLACE] * 6,
        [
            pltpu.SMEM((requests,), jnp.int32),
            pltpu.SMEM((requests,), jnp.int32),
            pltpu.VMEM((requests, width), bf16),
            pltpu.VMEM((width,), bf16),
            pltpu.VMEM((requests, rank, width), bf16),
            dma((4,)),
            dma((requests,)),
            dma((requests,)),
        ],
    )(
        adapter_choice_index,
        lengths,
        hidden_state_input,
        attention_norm_gain,
        adapter_down_matrix,
        adapter_up_matrix,
    )
    small = called(
        repeat_kernel,
        sds((everyone,) + small.shape, f32),
        [IN_VMEM],
        flops=covering,
        read=covering >> 10,
    )(small)
    small = lax.all_to_all(small, ("seq", "head"), 0, 0, tiled=True)
    parts = called(
        functools.partial(query_parts_kernel, width * devices, own_rows, own_kv),
        sds((targets * parts_rows, head_dim), bf16),
        [IN_VMEM] * 7,
        [
            pltpu.VMEM(((heads + 2 * kv_heads) * requests, head_dim), f32),
            pltpu.VMEM((targets * parts_rows, head_dim), f32),
        ],
        flops=covering,
        read=covering >> 10,
    )(
        owned,
        small,
        scaled,
        query_projection_matrix,
        key_projection_matrix,
        value_projection_matrix,
        up_rows,
    )
    parts = exchanged(parts, axes).reshape(devices, halves * parts_rows, head_dim)
    spread, own = called(
        functools.partial(rotation_kernel, own_rows, own_kv),
        (
            sds((devices, halves * own_rows, head_dim), bf16),
            sds((2, halves * own_rows, head_dim), f32),
        ),
        [IN_VMEM, IN_VMEM],
        flops=covering,
        read=covering >> 10,
    )(table, parts)
    query_rot = exchanged(spread.reshape(-1, head_dim), axes)

    entries = cached * kv_heads
    parts = called(
        functools.partial(attention_kernel, kv_heads, own_rows),
        sds((targets * (own_rows + 2), head_dim), bf16),
        [IN_VMEM] * 4,
        [
            pltpu.VMEM((requests, heads, entries), bf16),
            pltpu.VMEM((requests, heads, head_dim), f32),
            pltpu.VMEM((targets * (own_rows + 2), head_dim), f32),
        ],
        flops=4 * requests * heads * entries * head_dim,
        read=16 << 20,
    )(
        limits,
        query_rot,
        rotated_key_cache.reshape(requests, entries, head_dim),
        cached_value_rows.reshape(requests, entries, head_dim),
    )
    parts = exchanged(parts, axes)
    spread = called(
        functools.partial(combine_kernel, own_rows),
        sds((devices, halves * own_rows, head_dim), bf16),
        [IN_VMEM, IN_VMEM],
        [pltpu.VMEM(parts.shape, f32)],
    )(parts, own)
    attended = exchanged(spread.reshape(-1, head_dim), axes)
    out_columns = output_projection_matrix.shape[1]
    out_part = called(
        output_kernel,
        sds((requests, out_columns), f32),
        [IN_VMEM, IN_VMEM],
        [pltpu.VMEM((requests * heads, head_dim), f32)],
    )(attended, output_projection_matrix)
    if head_size == 2:
        output_sum = out_part + lax.ppermute(out_part, "head", [(0, 1), (1, 0)])
    else:
        output_sum = lax.psum(out_part, "head")
    return output_sum.astype(jnp.bfloat16)


def solution(mesh):
    return jax.shard_map(
        body,
        mesh=mesh,
        in_specs=(
            P(None, "seq"),
            P("seq"),
            P("seq", "head"),
            P("seq", "head"),
            P("seq", "head"),
            P("head", "seq"),
            P("head", None, "seq"),
            P("seq", None, "head"),
            P(),
            P(),
            P(None, "seq", "head", None),
            P(None, "seq", "head", None),
        ),
        out_specs=P(None, "seq"),
        check_vma=False,
    )
```

```python
import functools
import math

import jax
import jax.numpy as jnp
from jax import lax
from jax.experimental import pallas as pl
from jax.experimental.pallas import tpu as pltpu
from jax.sharding import PartitionSpec as P

norm_epsilon = 1e-05
adapter_scale_factor = 1.0
rope_base = 500000.0
masked_score = -1e30
masked_limit = 5e29

IN_VMEM = pl.BlockSpec(memory_space=pltpu.VMEM)
IN_PLACE = pl.BlockSpec(memory_space=pltpu.HBM)


def exchanged(rows, axes):
    count, head_dim = lax.axis_size(axes), rows.shape[1]
    inner = math.gcd(rows.shape[0] // count, 8)
    blocks = rows.reshape(count, -1, inner, head_dim)
    return lax.all_to_all(blocks, axes, 0, 0, tiled=True).reshape(rows.shape)


def iota(shape, axis):
    return lax.broadcasted_iota(jnp.int32, shape, axis)


def rounded(value):
    return value.astype(jnp.bfloat16).astype(jnp.float32)


def started(source, target, sem):
    copy = pltpu.make_async_copy(source, target, sem)
    copy.start()
    return copy


def owned_column(choice_ref, first, count):
    requests = choice_ref.shape[0]
    row = iota((requests, 1), 0)
    column = jnp.zeros((requests, 1), jnp.int32)
    for r in range(requests):
        local = choice_ref[r] - first
        held = ((local >= 0) & (local < count)).astype(jnp.int32)
        column = jnp.where(row == r, held, column)
    return column > 0


def small_sums_kernel(
    axes,
    own_rows,
    choice_hbm,
    lengths_hbm,
    hidden_hbm,
    gain_hbm,
    down_ref,
    up_ref,
    message_ref,
    scaled_ref,
    up_rows_ref,
    owned_ref,
    table_ref,
    limits_ref,
    choice_ref,
    lengths_ref,
    hidden_ref,
    gain_ref,
    down_rows_ref,
    sems,
    down_sems,
    up_sems,
):
    requests, rank, width = down_rows_ref.shape
    columns, head_dim = up_ref.shape[2], table_ref.shape[1]
    choice_copy = started(choice_hbm, choice_ref, sems.at[0])
    lengths_copy = started(lengths_hbm, lengths_ref, sems.at[1])
    hidden_copy = started(hidden_hbm, hidden_ref, sems.at[2])
    gain_copy = started(gain_hbm, gain_ref, sems.at[3])
    head_index = lax.axis_index("head")
    down_count, up_count = down_ref.shape[0], up_ref.shape[0]
    down_first = head_index * down_count
    up_first = lax.axis_index("seq") * up_count

    def up_copy(r):
        local = choice_ref[r] - up_first
        return pltpu.make_async_copy(up_ref.at[local], up_rows_ref.at[r], up_sems.at[r])

    def up_held(r):
        local = choice_ref[r] - up_first
        return (local >= 0) & (local < up_count)

    choice_copy.wait()
    down_copies = []
    for r in range(requests):
        local = jnp.clip(choice_ref[r] - down_first, 0, down_count - 1)
        down_copies.append(started(down_ref.at[local], down_rows_ref.at[r], down_sems.at[r]))
    for r in range(requests):

        @pl.when(up_held(r))
        def _(r=r):
            up_copy(r).start()

        @pl.when(jnp.logical_not(up_held(r)))
        def _(r=r):
            up_rows_ref[r] = jnp.zeros(up_rows_ref.shape[1:], up_rows_ref.dtype)

    owned_ref[...] = jnp.broadcast_to(
        owned_column(choice_ref, up_first, up_count).astype(jnp.float32), owned_ref.shape
    )
    lengths_copy.wait()
    for r in range(requests):
        limits_ref[pl.ds(r, 1), :] = jnp.full((1, limits_ref.shape[1]), lengths_ref[r], jnp.int32)
    own_request = lax.axis_index(axes) * own_rows // (columns // head_dim)
    position = lengths_ref[own_request].astype(jnp.float32)
    half_dim = head_dim // 2
    lane = iota((1, head_dim), 1)
    step = jnp.where(lane < half_dim, lane, lane - half_dim).astype(jnp.float32)
    angles = position * jnp.exp(-step * (math.log(rope_base) / half_dim))
    sine_val = jnp.sin(angles)
    table_ref[0:1, :] = jnp.cos(angles)
    table_ref[1:2, :] = jnp.where(lane < half_dim, -sine_val, sine_val)

    hidden_copy.wait()
    gain_copy.wait()
    values = hidden_ref[...].astype(jnp.float32)
    gain = gain_ref[...].astype(jnp.float32).reshape(1, width)
    scaled = (values * gain).astype(jnp.bfloat16)
    scaled_ref[...] = scaled
    squares = jnp.sum(values * values, axis=1, keepdims=True)
    squares = jnp.where(head_index == 0, squares, 0.0)
    diagonal = iota((requests, 128), 1) == iota((requests, 128), 0)
    squares = jnp.sum(jnp.where(diagonal, squares, 0.0), axis=0, keepdims=True)
    owned = owned_column(choice_ref, down_first, down_count)
    for copy in down_copies:
        copy.wait()
    products = lax.dot_general(
        scaled,
        down_rows_ref[...].reshape(requests * rank, width),
        (((1,), (1,)), ((), ())),
        preferred_element_type=jnp.float32,
    )
    keep = (iota(products.shape, 1) // rank == iota(products.shape, 0)) & owned
    sums = jnp.sum(jnp.where(keep, products, 0.0), axis=0, keepdims=True)
    message = jnp.concatenate([sums, squares], axis=1)
    message_ref[...] = message
    for r in range(requests):

        @pl.when(up_held(r))
        def _(r=r):
            up_copy(r).wait()


def repeat_kernel(message_ref, repeated_ref):
    repeated_ref[...] = jnp.broadcast_to(message_ref[...][None], repeated_ref.shape)


def query_parts_kernel(
    model_width,
    own_rows,
    own_kv,
    owned_ref,
    small_ref,
    scaled_ref,
    query_ref,
    key_ref,
    value_ref,
    up_rows_ref,
    message_ref,
    rows_ref,
    staged_ref,
):
    requests, rank, columns = up_rows_ref.shape
    head_dim = message_ref.shape[1]
    heads = columns // head_dim
    kv_heads = key_ref.shape[1] // head_dim
    small = jnp.sum(small_ref[...], axis=0)
    sums, squares = small[:, : requests * rank], small[:, requests * rank :]
    diagonal = iota((requests, 128), 1) == iota((requests, 128), 0)
    squares = jnp.sum(jnp.where(diagonal, squares, 0.0), axis=1, keepdims=True)
    inverse = lax.rsqrt(squares / model_width + norm_epsilon)
    shape = (requests, requests * rank)
    keep = (iota(shape, 1) // rank == iota(shape, 0)) & (owned_ref[:, 0:1] > 0)
    shrunk = sums * inverse * adapter_scale_factor
    shrunk = jnp.where(keep, shrunk, 0.0).astype(jnp.bfloat16)
    scaled = scaled_ref[...]
    up_rows = up_rows_ref.reshape(requests * rank, columns)
    chunk = min(columns, 1024)
    query_places = list(range(heads))
    key_places = [heads + k + k // own_kv * own_kv for k in range(kv_heads)]
    value_places = [place + own_kv for place in key_places]
    places = iter(query_places + key_places + value_places)
    for weight_ref in (query_ref, key_ref, value_ref):
        for start in range(0, weight_ref.shape[1], chunk):
            size = min(chunk, weight_ref.shape[1] - start)
            part = jnp.dot(
                scaled, weight_ref[:, pl.ds(start, size)], preferred_element_type=jnp.float32
            )
            part = part * inverse
            if weight_ref is query_ref:
                part = part + jnp.dot(
                    shrunk, up_rows[:, pl.ds(start, size)], preferred_element_type=jnp.float32
                )
            for k in range(size // head_dim):
                rows_ref[pl.ds(next(places) * requests, requests), :] = part[
                    :, k * head_dim : (k + 1) * head_dim
                ]
    rows = own_rows + 2 * own_kv
    for t in range(requests * heads // own_rows):
        r, h = divmod(t * own_rows, heads)
        kv = heads + 2 * (h * kv_heads // heads)
        staged_ref[pl.ds(t * rows, own_rows), :] = rows_ref[
            pl.ds(h * requests + r, own_rows, stride=requests), :
        ]
        staged_ref[pl.ds(t * rows + own_rows, 2 * own_kv), :] = rows_ref[
            pl.ds(kv * requests + r, 2 * own_kv, stride=requests), :
        ]
    message_ref[...] = staged_ref[...].astype(jnp.bfloat16)


def rotation_kernel(own_rows, own_kv, table_ref, parts_ref, spread_ref, own_ref):
    head_dim = spread_ref.shape[2]
    group = own_rows // own_kv
    rows = own_rows + 2 * own_kv
    sums = jnp.sum(parts_ref[...].astype(jnp.float32), axis=0)
    cosine, sine_val = table_ref[0:1, :], table_ref[1:2, :]
    rotated = rounded(sums * cosine + pltpu.roll(sums, head_dim // 2, 1) * sine_val)

    def repeated(rows, first):
        return [
            jnp.broadcast_to(rows[first + k : first + k + 1], (group, head_dim))
            for k in range(own_kv)
        ]

    queries, keys, values = [], [], []
    for first in range(0, sums.shape[0], rows):
        queries.append(rotated[first : first + own_rows])
        keys += repeated(rotated, first + own_rows)
        values += repeated(rounded(sums), first + own_rows + own_kv)
    query_rot = jnp.concatenate(queries)
    spread_ref[...] = jnp.broadcast_to(query_rot.astype(jnp.bfloat16)[None], spread_ref.shape)
    own_score = jnp.sum(query_rot * jnp.concatenate(keys), axis=1, keepdims=True)
    own_ref[0] = jnp.broadcast_to(own_score * head_dim ** (-0.5), query_rot.shape)
    own_ref[1] = jnp.concatenate(values)


def attention_kernel(
    kv_heads,
    own_rows,
    limits_ref,
    query_ref,
    key_ref,
    value_ref,
    message_ref,
    scores_ref,
    weights_ref,
    stats_ref,
    staged_ref,
):
    requests, entries, head_dim = key_ref.shape
    cached = entries // kv_heads
    heads = query_ref.shape[0] // requests
    group = heads // kv_heads
    first = lax.axis_index("seq") * cached
    lane = iota((heads, head_dim), 1)
    row = iota((heads, head_dim), 0)
    per_tile = head_dim // kv_heads
    position = jnp.where(
        lane % kv_heads == row // group, first + lane // kv_heads, jnp.int32(2**30)
    )
    score_scale = head_dim ** (-0.5)
    for r in range(requests):
        scores_ref[r] = lax.dot_general(
            query_ref[pl.ds(r * heads, heads), :],
            key_ref[r],
            (((1,), (1,)), ((), ())),
            preferred_element_type=jnp.float32,
        )
    for r in range(requests):
        limit = limits_ref[pl.ds(r, 1), :]
        tiles = []
        peak = jnp.full((heads, head_dim), -masked_limit, jnp.float32)
        for c in range(entries // head_dim):
            valid = position < limit - c * per_tile
            tile = scores_ref[r, :, pl.ds(c * head_dim, head_dim)]
            tiles.append(jnp.where(valid, tile, masked_score))
            peak = jnp.maximum(peak, tiles[-1])
        peak = jnp.max(peak, axis=1, keepdims=True)
        total = jnp.zeros((heads, head_dim), jnp.float32)
        for c, tile in enumerate(tiles):
            weights = jnp.exp2((tile - peak) * (score_scale * math.log2(math.e)))
            total = total + weights
            weights_ref[r, :, pl.ds(c * head_dim, head_dim)] = weights.astype(jnp.bfloat16)
        total = jnp.sum(total, axis=1, keepdims=True)
        peak = peak * score_scale
        peak_high = rounded(peak)
        peak_mid = rounded(peak - peak_high)
        peak_low = peak - peak_high - peak_mid
        total_high = rounded(total)
        total_low = rounded(total - total_high)
        stats = jnp.zeros((heads, head_dim), jnp.float32)
        for k, piece in enumerate((peak_high, peak_mid, peak_low, total_high, total_low)):
            stats = jnp.where(lane == k * own_rows + row % own_rows, piece, stats)
        stats_ref[r] = stats
    for r in range(requests):
        out = jnp.dot(weights_ref[r], value_ref[r], preferred_element_type=jnp.float32)
        for part in range(heads // own_rows):
            window = slice(part * own_rows, (part + 1) * own_rows)
            place = (r * (heads // own_rows) + part) * (own_rows + 2)
            stats_row = jnp.sum(stats_ref[r, window, :], axis=0, keepdims=True)
            staged_ref[pl.ds(place, own_rows), :] = out[window]
            staged_ref[pl.ds(place + own_rows, 2), :] = jnp.broadcast_to(stats_row, (2, head_dim))
    message_ref[...] = staged_ref[...].astype(jnp.bfloat16)


def combine_kernel(own_rows, parts_ref, own_ref, spread_ref, staged_ref):
    devices, all_rows, head_dim = spread_ref.shape
    halves = all_rows // own_rows
    lane = iota((own_rows, head_dim), 1)
    row = iota((own_rows, head_dim), 0)
    staged_ref[...] = parts_ref[...].astype(jnp.float32)
    same_row = lane % own_rows == row
    for half in range(halves):
        window = slice(half * own_rows, (half + 1) * own_rows)
        own_score = own_ref[0, window, 0:1]
        places = [(s * halves + half) * (own_rows + 2) for s in range(devices)]
        peaks, totals = [], []
        overall = own_score
        for place in places:
            stats = staged_ref[pl.ds(place + own_rows, 1), :]
            stats = jnp.where(same_row & (lane < 5 * own_rows), stats, 0.0)
            peak = jnp.where(lane < 3 * own_rows, stats, 0.0)
            peaks.append(jnp.sum(peak, axis=1, keepdims=True))
            total = jnp.where(lane < 3 * own_rows, 0.0, stats)
            totals.append(jnp.sum(total, axis=1, keepdims=True))
            overall = jnp.maximum(overall, peaks[-1])
        own_weight = jnp.exp(own_score - overall)
        denominator = own_weight
        summed = own_weight * own_ref[1, window, :]
        for place, peak, total in zip(places, peaks, totals):
            factor = jnp.exp(peak - overall)
            denominator = denominator + total * factor
            summed = summed + factor * staged_ref[pl.ds(place, own_rows), :]
        attended = (summed / denominator).astype(jnp.bfloat16)
        spread_ref[:, window, :] = jnp.broadcast_to(
            attended[None], (devices, own_rows, head_dim)
        )


def output_kernel(attended_ref, weight_ref, out_ref, rows_ref):
    requests = out_ref.shape[0]
    heads = attended_ref.shape[0] // requests
    rows_ref[...] = attended_ref[...].astype(jnp.float32)
    left = jnp.concatenate(
        [rows_ref[pl.ds(h, requests, stride=heads), :] for h in range(heads)], axis=1
    ).astype(jnp.bfloat16)
    out_ref[...] = jnp.dot(left, weight_ref[...], preferred_element_type=jnp.float32)


def called(kernel, out_shape, in_specs, scratch=(), flops=0, read=0):
    call = pl.pallas_call(
        kernel,
        out_shape=out_shape,
        in_specs=in_specs,
        out_specs=jax.tree.map(lambda _: IN_VMEM, out_shape),
        scratch_shapes=list(scratch),
        cost_estimate=pl.CostEstimate(flops=flops, transcendentals=0, bytes_accessed=read),
        compiler_params=pltpu.CompilerParams(vmem_limit_bytes=16 << 20),
    )

    def run(*operands):
        return call(
            *(
                pltpu.with_memory_space_constraint(operand, pltpu.HBM)
                if spec is IN_PLACE
                else operand
                for operand, spec in zip(operands, in_specs, strict=True)
            )
        )

    return run


def body(
    hidden_state_input,
    attention_norm_gain,
    query_projection_matrix,
    key_projection_matrix,
    value_projection_matrix,
    output_projection_matrix,
    adapter_down_matrix,
    adapter_up_matrix,
    adapter_choice_index,
    lengths,
    rotated_key_cache,
    cached_value_rows,
):
    f32, bf16 = jnp.float32, jnp.bfloat16
    requests, width = hidden_state_input.shape
    _, cached, kv_heads, head_dim = rotated_key_cache.shape
    columns = query_projection_matrix.shape[1]
    heads = columns // head_dim
    rank = adapter_down_matrix.shape[1]
    devices = lax.axis_size("seq")
    head_size = lax.axis_size("head")
    everyone = devices * head_size
    group = heads // kv_heads
    shared = requests * heads % everyone == 0
    axes = ("seq", "head") if shared else ("seq",)
    halves = head_size if shared else 1
    own_rows = requests * heads // (devices * halves)
    own_kv = max(own_rows // group, 1)
    parts_rows = own_rows + 2 * own_kv
    targets = devices * halves
    covering = 16 << 30
    sds = jax.ShapeDtypeStruct
    dma = pltpu.SemaphoreType.DMA

    small, scaled, up_rows, owned, table, limits = called(
        functools.partial(small_sums_kernel, axes, own_rows),
        (
            sds((1, requests * rank + 128), f32),
            sds((requests, width), bf16),
            sds((requests, rank, columns), bf16),
            sds((requests, 128), f32),
            sds((2, head_dim), f32),
            sds((requests, 128), jnp.int32),
        ),
        [IN_PLACE] * 6,
        [
            pltpu.SMEM((requests,), jnp.int32),
            pltpu.SMEM((requests,), jnp.int32),
            pltpu.VMEM((requests, width), bf16),
            pltpu.VMEM((width,), bf16),
            pltpu.VMEM((requests, rank, width), bf16),
            dma((4,)),
            dma((requests,)),
            dma((requests,)),
        ],
    )(
        adapter_choice_index,
        lengths,
        hidden_state_input,
        attention_norm_gain,
        adapter_down_matrix,
        adapter_up_matrix,
    )
    small = called(
        repeat_kernel,
        sds((everyone,) + small.shape, f32),
        [IN_VMEM],
        flops=covering,
        read=covering >> 10,
    )(small)
    small = lax.all_to_all(small, ("seq", "head"), 0, 0, tiled=True)
    parts = called(
        functools.partial(query_parts_kernel, width * devices, own_rows, own_kv),
        sds((targets * parts_rows, head_dim), bf16),
        [IN_VMEM] * 7,
        [
            pltpu.VMEM(((heads + 2 * kv_heads) * requests, head_dim), f32),
            pltpu.VMEM((targets * parts_rows, head_dim), f32),
        ],
        flops=covering,
        read=covering >> 10,
    )(
        owned,
        small,
        scaled,
        query_projection_matrix,
        key_projection_matrix,
        value_projection_matrix,
        up_rows,
    )
    parts = exchanged(parts, axes).reshape(devices, halves * parts_rows, head_dim)
    spread, own = called(
        functools.partial(rotation_kernel, own_rows, own_kv),
        (
            sds((devices, halves * own_rows, head_dim), bf16),
            sds((2, halves * own_rows, head_dim), f32),
        ),
        [IN_VMEM, IN_VMEM],
        flops=covering,
        read=covering >> 10,
    )(table, parts)
    query_rot = exchanged(spread.reshape(-1, head_dim), axes)

    entries = cached * kv_heads
    parts = called(
        functools.partial(attention_kernel, kv_heads, own_rows),
        sds((targets * (own_rows + 2), head_dim), bf16),
        [IN_VMEM] * 4,
        [
            pltpu.VMEM((requests, heads, entries), f32),
            pltpu.VMEM((requests, heads, entries), bf16),
            pltpu.VMEM((requests, heads, head_dim), f32),
            pltpu.VMEM((targets * (own_rows + 2), head_dim), f32),
        ],
        flops=4 * requests * heads * entries * head_dim,
        read=16 << 20,
    )(
        limits,
        query_rot,
        rotated_key_cache.reshape(requests, entries, head_dim),
        cached_value_rows.reshape(requests, entries, head_dim),
    )
    parts = exchanged(parts, axes)
    spread = called(
        functools.partial(combine_kernel, own_rows),
        sds((devices, halves * own_rows, head_dim), bf16),
        [IN_VMEM, IN_VMEM],
        [pltpu.VMEM(parts.shape, f32)],
    )(parts, own)
    attended = exchanged(spread.reshape(-1, head_dim), axes)
    out_columns = output_projection_matrix.shape[1]
    out_part = called(
        output_kernel,
        sds((requests, out_columns), f32),
        [IN_VMEM, IN_VMEM],
        [pltpu.VMEM((requests * heads, head_dim), f32)],
    )(attended, output_projection_matrix)
    if head_size == 2:
        output_sum = out_part + lax.ppermute(out_part, "head", [(0, 1), (1, 0)])
    else:
        output_sum = lax.psum(out_part, "head")
    return output_sum.astype(jnp.bfloat16)


def solution(mesh):
    return jax.shard_map(
        body,
        mesh=mesh,
        in_specs=(
            P(None, "seq"),
            P("seq"),
            P("seq", "head"),
            P("seq", "head"),
            P("seq", "head"),
            P("head", "seq"),
            P("head", None, "seq"),
            P("seq", None, "head"),
            P(),
            P(),
            P(None, "seq", "head", None),
            P(None, "seq", "head", None),
        ),
        out_specs=P(None, "seq"),
        check_vma=False,
    )
```
